32 devices in a mesh: aux: 16 (over z, y, x), ao: 2 (over core).
Axes of the slice: x: 2, y: 2, z: 4, core: 2. Of those that a mesh axis runs over, the one named last changes fastest.
Arguments:
- ints: bfloat16 [256, 768, 768], P('aux', 'ao'), may hold values from -1.25 to 1.25
- occ_coef: bfloat16 [768, 32], replicated, may hold values from -0.21875 to 0.21875
- vir_coef: bfloat16 [768, 512], P('ao'), may hold values from -0.21875 to 0.21875
- occ_energy: float32 [32], replicated, may hold values from -2 to -0.3
- vir_energy: float32 [512], replicated, may hold values from 0.3 to 3
Outputs:
- density: float32 [32, 512, 512], P('aux', 'ao')
The draws below stay inside these ranges and needn't reach their ends.
All inputs are finite; a program needn't handle non-finite values.
Results may differ from the reference program's by a relative error of at most 0.0065.
Values may be sent and summed in bfloat16 or wider, within the bound.
A program may use at most 128 MiB of HBM per device.

```python
import jax
import jax.numpy as jnp
from jax import lax

AO = 768
NVIR = 512
OCC_DEV = 2
CYCLE = 4
NOCC = 32
NAUX = 256
N_AUX = 16


def block_scale(stream_key, extent, pieces, least, top_value):
    gain, own = 1.0, jax.random.fold_in(stream_key, 6)
    for axis_at, blocks in pieces:
        heights = jnp.exp(jax.random.uniform(jax.random.fold_in(own, axis_at), (blocks,), jnp.float32, least / len(pieces), top_value / len(pieces)))
        gain = gain * jnp.repeat(heights, extent[axis_at] // blocks).reshape([-1 if axis == axis_at else 1 for axis in range(len(extent))])
    return gain


def centred(own_key, dims, width, bound, cuts=(), held_as=jnp.bfloat16):
    level = block_scale(own_key, dims, cuts, -0.22, 0.18) if cuts else 1.0
    drawn = jax.random.normal(own_key, dims, jnp.float32) * width * level
    return jnp.minimum(jnp.maximum(drawn, -bound), bound).astype(held_as)


def setup_inputs(seed: int = 0) -> dict:
    key_list = jax.random.split(jax.random.key(seed), 6)
    ints = centred(key_list[0], (NAUX, AO, AO), 0.08, 1.25, ((0, 16), (1, 2)))
    occ_coef = centred(key_list[1], (AO, NOCC), AO ** -0.5, 0.21875)
    vir_coef = centred(key_list[2], (AO, NVIR), AO ** -0.5, 0.21875, ((0, 2),))
    occ_energy = jnp.clip(jax.random.uniform(key_list[3], (NOCC,), jnp.float32, -2.0, -0.3), -2.0, -0.3)
    vir_energy = jnp.clip(jax.random.uniform(key_list[4], (NVIR,), jnp.float32, 0.3, 3.0), 0.3, 3.0)
    return {"ints": ints, "occ_coef": occ_coef, "vir_coef": vir_coef, "occ_energy": occ_energy, "vir_energy": vir_energy}


def reference(ints, occ_coef, vir_coef, occ_energy, vir_energy):
    def transform(slab):
        half_ints = jnp.dot(slab, occ_coef, preferred_element_type=jnp.float32).astype(jnp.bfloat16)
        return jnp.dot(half_ints.T, vir_coef, preferred_element_type=jnp.float32).astype(jnp.bfloat16)

    three = lax.map(transform, ints)
    offsets = jnp.arange(2 * CYCLE + 1, dtype=jnp.int32) - CYCLE
    inside = jnp.arange(OCC_DEV, dtype=jnp.int32)
    vir_pairs = vir_energy[:, None] + vir_energy[None, :]

    def one_orbital(orbital):
        block_index = orbital // OCC_DEV
        blocks = (block_index + offsets + N_AUX) % N_AUX
        partners = (blocks[:, None] * OCC_DEV + inside[None, :]).reshape(-1).astype(jnp.int32)
        partner_rows = jnp.take(three, partners, axis=1).astype(jnp.float32)
        own_rows = lax.dynamic_index_in_dim(three, orbital, 1, keepdims=False).astype(jnp.float32)
        integrals = jnp.einsum("qa,qjb->jab", own_rows, partner_rows)
        own_energy = lax.dynamic_index_in_dim(occ_energy, orbital, 0, keepdims=False)
        pair_energy = jnp.take(occ_energy, partners, axis=0)
        energy_gap = own_energy + pair_energy[:, None, None] - vir_pairs[None]
        scaled = integrals / energy_gap
        amplitude = scaled.astype(jnp.bfloat16).astype(jnp.float32)
        mixed = (2.0 * scaled - jnp.swapaxes(scaled, 1, 2)).astype(jnp.bfloat16).astype(jnp.float32)
        return jnp.einsum("jac,jbc->ab", amplitude, mixed)

    return lax.map(one_orbital, jnp.arange(NOCC, dtype=jnp.int32))
```

```python
import functools

import jax
import jax.numpy as jnp
from jax import lax
from jax.experimental import pallas as pl
from jax.experimental.pallas import tpu as pltpu
from jax.sharding import PartitionSpec as P

CYCLE = 4
MESH = pl.DeviceIdType.MESH
NT = (((1,), (1,)), ((), ()))


def places(me, aux_count):
    layers = aux_count // CYCLE
    layer, place = lax.div(me, CYCLE), lax.rem(me, CYCLE)
    column, row = lax.rem(place, 2), lax.div(place, 2)
    base = layer * CYCLE
    beside = base + place + 1 - 2 * column
    along = base + place + 2 - 4 * row
    across = base + CYCLE - 1 - place
    above = lax.rem(me + CYCLE, aux_count)
    below = lax.rem(me + aux_count - CYCLE, aux_count)
    last = jnp.where(layer == layers - 1, 1, 0)
    return column, row, beside, along, across, above, below, last


def pairs_kernel(
    aux_count, share, own_ref, occ_ref, vir_row_ref, vir_col_ref, out_ref,
    slots, own_t, vis_t, vir_pairs, amp, mix, acc, outgoing, incoming,
    send_sems, recv_sems, swap_sems,
):
    me = lax.axis_index("aux")
    core = lax.axis_index("ao")
    other = 1 - core
    block, _, nvir = own_ref.shape
    half = nvir // 2
    slot_count = 2 * CYCLE + 1
    column, row, beside, along, across, above, below, last = places(me, aux_count)

    barrier = pltpu.get_barrier_semaphore()
    for target in (beside, along, across, above, below):
        pl.semaphore_signal(barrier, inc=1, device_id=(target, core), device_id_type=MESH)
    pl.semaphore_signal(barrier, inc=1, device_id=(me, other), device_id_type=MESH)
    pl.semaphore_wait(barrier, 6)

    def remote(source, slot, target):
        return pltpu.make_async_remote_copy(
            src_ref=source,
            dst_ref=slots.at[slot],
            send_sem=send_sems.at[slot],
            recv_sem=recv_sems.at[slot],
            device_id=(target, core),
            device_id_type=MESH,
        )

    def arrived(slot):
        pltpu.make_async_copy(slots.at[slot], slots.at[slot], recv_sems.at[slot]).wait()

    piece = own_ref.at[pl.ds(core * share, share)]
    first = jnp.where(last == 1, below, above)
    second = jnp.where(last == 1, above, below)
    remote(piece, 1, beside).start()
    remote(piece, 2, along).start()
    remote(piece, 5 - last, first).start()
    remote(piece, 3, across).start()
    remote(piece, 4 + last, second).start()
    pltpu.make_async_copy(piece, slots.at[0], recv_sems.at[0]).start()
    beside_source, along_source = 4 + column, 4 + row
    beyond = jnp.where(row == 0, above, below)

    for i in range(block):
        own_t[i] = own_ref[i].T
    vir_pairs[...] = vir_col_ref[...] + vir_row_ref[...]
    acc[...] = jnp.zeros_like(acc)

    near, far = 4 + last, 5 - last

    def forward(source):
        @pl.when(beside_source == source)
        def _():
            remote(slots.at[source], 6, beside).start()

        @pl.when(along_source == source)
        def _():
            remote(slots.at[source], 7, along).start()

    def visit(step, carry):
        slot = jnp.where(step == 1, near, jnp.where(step == 4, far, jnp.where(step == 5, 3, step)))
        slot = jnp.where(step == 2, 1, jnp.where(step == 3, 2, slot))

        @pl.when(step != 5)
        def _():
            arrived(slot)

        @pl.when(step == 1)
        def _():
            forward(near)

        @pl.when(step == 4)
        def _():
            forward(far)
            arrived(3)
            remote(slots.at[3], 8, beyond).start()

        to_owner = jnp.where(slot == 0, me, jnp.where(slot == 1, beside, jnp.where(slot == 2, along, across)))
        from_beside = jnp.where(column == 1, beside + CYCLE, beside + aux_count - CYCLE)
        from_along = jnp.where(row == 1, along + CYCLE, along + aux_count - CYCLE)
        from_beyond = jnp.where(row == 1, across + CYCLE, across + aux_count - CYCLE)
        forwarded = jnp.where(slot == 6, from_beside, jnp.where(slot == 7, from_along, from_beyond))
        forwarded = lax.rem(forwarded, aux_count)
        stacked = jnp.where(slot == 4, above, below)
        owner = jnp.where(slot < 4, to_owner, jnp.where(slot < 6, stacked, forwarded))
        for s in range(share):
            pair_energy = occ_ref[owner * block + core * share + s]
            visitor = slots[slot, s]
            vis_t[...] = visitor.T
            for i in range(block):
                energy = occ_ref[me * block + i] + pair_energy
                for t in range(2):
                    rows = slice(t * half, (t + 1) * half)
                    direct = jnp.dot(own_t[i, rows], visitor, preferred_element_type=jnp.float32)
                    swapped = jnp.dot(vis_t[rows], own_ref[i], preferred_element_type=jnp.float32)
                    inverse = 1.0 / (energy - vir_pairs[rows])
                    amp[i, rows] = (direct * inverse).astype(jnp.bfloat16)
                    mix[i, rows] = ((2.0 * direct - swapped) * inverse).astype(jnp.bfloat16)
                acc[i] += lax.dot_general(amp[i], mix[i], NT, preferred_element_type=jnp.float32)
        return carry

    lax.fori_loop(0, slot_count, visit, 0)

    outgoing[...] = acc[:, pl.ds(pl.multiple_of(other * half, half), half)].astype(jnp.bfloat16)
    swap = pltpu.make_async_remote_copy(
        src_ref=outgoing,
        dst_ref=incoming,
        send_sem=swap_sems.at[0],
        recv_sem=swap_sems.at[1],
        device_id=(me, other),
        device_id_type=MESH,
    )
    swap.start()
    for slot in range(1, slot_count):
        remote(piece, slot, beside).wait_send()
    swap.wait()
    kept = acc[:, pl.ds(pl.multiple_of(core * half, half), half)]
    out_ref[...] = kept + incoming[...].astype(jnp.float32)


def pair_densities(own_block, occ_energy, vir_energy, aux_count, share):
    block, naux, nvir = own_block.shape
    half = nvir // 2
    slot_count = 2 * CYCLE + 1
    vmem = pl.BlockSpec(memory_space=pltpu.VMEM)
    return pl.pallas_call(
        functools.partial(pairs_kernel, aux_count, share),
        out_shape=jax.ShapeDtypeStruct((block, half, nvir), jnp.float32),
        in_specs=[vmem, pl.BlockSpec(memory_space=pltpu.SMEM), vmem, vmem],
        out_specs=vmem,
        scratch_shapes=[
            pltpu.VMEM((slot_count, share, naux, nvir), jnp.bfloat16),
            pltpu.VMEM((block, nvir, naux), jnp.bfloat16),
            pltpu.VMEM((nvir, naux), jnp.bfloat16),
            pltpu.VMEM((nvir, nvir), jnp.float32),
            pltpu.VMEM((block, nvir, nvir), jnp.bfloat16),
            pltpu.VMEM((block, nvir, nvir), jnp.bfloat16),
            pltpu.VMEM((block, nvir, nvir), jnp.float32),
            pltpu.VMEM((block, half, nvir), jnp.bfloat16),
            pltpu.VMEM((block, half, nvir), jnp.bfloat16),
            pltpu.SemaphoreType.DMA((slot_count,)),
            pltpu.SemaphoreType.DMA((slot_count,)),
            pltpu.SemaphoreType.DMA((2,)),
        ],
        compiler_params=pltpu.CompilerParams(collective_id=0, has_side_effects=True, vmem_limit_bytes=48 * 2**20),
    )(own_block, occ_energy, vir_energy[None, :], vir_energy[:, None])


def shards(ints, occ_coef, vir_coef, occ_energy, vir_energy):
    core = lax.axis_index("ao")
    aux_count = lax.axis_size("aux")
    ao_count = lax.axis_size("ao")
    share = occ_coef.shape[1] // aux_count // ao_count
    half = vir_coef.shape[1] // ao_count
    half_ints = jnp.einsum(
        "qmn,ni->qmi", ints, occ_coef, preferred_element_type=jnp.float32
    ).astype(jnp.bfloat16)
    partial_sum = jnp.einsum("qmi,ma->qia", half_ints, vir_coef, preferred_element_type=jnp.float32)
    given = lax.dynamic_slice_in_dim(partial_sum, (1 - core) * half, half, 2).astype(jnp.bfloat16)
    taken = lax.ppermute(given, "ao", [(0, 1), (1, 0)])
    kept = lax.dynamic_slice_in_dim(partial_sum, core * half, half, 2)
    summed = (kept + taken.astype(jnp.float32)).astype(jnp.bfloat16)
    grouped = lax.all_to_all(summed, "aux", split_axis=1, concat_axis=0, tiled=True)
    own_block = lax.all_gather(grouped, "ao", axis=2, tiled=True)
    return pair_densities(
        jnp.swapaxes(own_block, 0, 1), occ_energy, vir_energy, aux_count, share
    )


def solution(mesh):
    return jax.shard_map(
        shards,
        mesh=mesh,
        in_specs=(P("aux", "ao", None), P(), P("ao", None), P(), P()),
        out_specs=P("aux", "ao", None),
        check_vma=False,
    )
```

```python
import functools

import jax
import jax.numpy as jnp
from jax import lax
from jax.experimental import pallas as pl
from jax.experimental.pallas import tpu as pltpu
from jax.sharding import PartitionSpec as P

CYCLE = 4
MESH = pl.DeviceIdType.MESH
NT = (((1,), (1,)), ((), ()))


def places(me, aux_count):
    layers = aux_count // CYCLE
    layer, place = lax.div(me, CYCLE), lax.rem(me, CYCLE)
    column, row = lax.rem(place, 2), lax.div(place, 2)
    base = layer * CYCLE
    beside = base + place + 1 - 2 * column
    along = base + place + 2 - 4 * row
    across = base + CYCLE - 1 - place
    above = lax.rem(me + CYCLE, aux_count)
    below = lax.rem(me + aux_count - CYCLE, aux_count)
    last = jnp.where(layer == layers - 1, 1, 0)
    return column, row, beside, along, across, above, below, last


def density_kernel(
    aux_count, share, ints_ref, occ_ref, vir_ref, occ_energy_ref, vir_energy_ref, out_ref,
    ints, occ_t, vir, occ_energy, vir_energy, half_ints, given, taken, kept, outbox, own,
    slots, own_t, vis_t, vir_pairs, amp, mix, acc, outgoing, incoming,
    load_sems, input_sems, give_sems, take_sems, spread_sems, join_sems,
    send_sems, recv_sems, swap_sems,
):
    me = lax.axis_index("aux")
    core = lax.axis_index("ao")
    other = 1 - core
    block, naux, nvir = own.shape
    groups, rows_in_group, nao = ints.shape
    chunks, norb, depth, half = outbox.shape
    part = half_ints.shape[2]
    held = chunks * depth
    slot_count = 2 * CYCLE + 1
    column, row, beside, along, across, above, below, last = places(me, aux_count)
    f32, bf16 = jnp.float32, jnp.bfloat16

    inputs = [
        pltpu.make_async_copy(source, target, input_sems.at[at])
        for at, (source, target) in enumerate(
            ((occ_ref, occ_t), (vir_ref, vir), (vir_energy_ref, vir_energy), (occ_energy_ref, occ_energy))
        )
    ]
    loads = [
        pltpu.make_async_copy(
            ints_ref.at[pl.ds(group * rows_in_group, rows_in_group)], ints.at[group], load_sems.at[group]
        )
        for group in range(groups)
    ]
    inputs[0].start()
    loads[0].start()
    for copy in inputs[1:] + loads[1:]:
        copy.start()

    barrier = pltpu.get_barrier_semaphore()

    def greet(step, carry):
        target = lax.rem(me + step, aux_count)
        pl.semaphore_signal(barrier, inc=1, device_id=(target, core), device_id_type=MESH)
        return carry

    lax.fori_loop(1, aux_count, greet, 0)
    pl.semaphore_signal(barrier, inc=1, device_id=(me, other), device_id_type=MESH)

    inputs[0].wait()
    occ = occ_t[...].T
    acc[...] = jnp.zeros_like(acc)
    inputs[1].wait()
    mine = pl.ds(pl.multiple_of(core * half, half), half)
    theirs = pl.ds(pl.multiple_of(other * half, half), half)
    to_row = lax.broadcasted_iota(jnp.int32, (norb * depth, norb * depth), 0)
    from_row = lax.broadcasted_iota(jnp.int32, (norb * depth, norb * depth), 1)
    order = jnp.where(from_row == lax.rem(to_row, depth) * norb + lax.div(to_row, depth), 1.0, 0.0).astype(bf16)

    def give(chunk):
        return pltpu.make_async_remote_copy(
            src_ref=given.at[chunk],
            dst_ref=taken.at[chunk],
            send_sem=give_sems.at[chunk],
            recv_sem=take_sems.at[chunk],
            device_id=(me, other),
            device_id_type=MESH,
        )

    def spread(chunk):
        give(chunk).wait_recv()
        total = kept[chunk] + taken[chunk].astype(f32)
        outbox[chunk] = total.astype(bf16).reshape(norb, depth, half)
        place = pl.ds(pl.multiple_of(me * held + chunk * depth, depth), depth)

        def send(step, carry):
            target = lax.rem(me + step, aux_count)
            pltpu.make_async_remote_copy(
                src_ref=outbox.at[chunk, pl.ds(target * block, block)],
                dst_ref=own.at[:, place, mine],
                send_sem=spread_sems.at[0],
                recv_sem=spread_sems.at[1],
                device_id=(target, core),
                device_id_type=MESH,
            ).start()
            return carry

        lax.fori_loop(1, aux_count, send, 0)
        pltpu.make_async_copy(
            outbox.at[chunk, pl.ds(me * block, block)], own.at[:, place, mine], spread_sems.at[1]
        ).start()

    in_chunk = groups // chunks
    in_group = rows_in_group // part
    cut = rows_in_group // 2
    for group in range(groups):
        chunk = group // in_chunk
        loads[group].wait()
        for piece in range(2):
            product = jnp.dot(ints[group, piece * cut : (piece + 1) * cut], occ, preferred_element_type=f32).astype(bf16)
            for q in range(in_group // 2):
                at = ((group % in_chunk) * in_group + piece * (in_group // 2) + q) * norb
                half_ints[chunk, at : at + norb] = product[q * part : (q + 1) * part].T
        if group % in_chunk == in_chunk - 1:
            ordered = jnp.dot(order, half_ints[chunk], preferred_element_type=f32).astype(bf16)
            given[chunk] = jnp.dot(ordered, vir[:, theirs], preferred_element_type=f32).astype(bf16)
            if chunk == 0:
                pl.semaphore_wait(barrier, aux_count)
            give(chunk).start()
            kept[chunk] = jnp.dot(ordered, vir[:, mine], preferred_element_type=f32)
        elif chunk > 0:
            spread(chunk - 1)
    spread(chunks - 1)

    inputs[2].wait()
    inputs[3].wait()
    lanes = 128
    column_energy = jnp.broadcast_to(vir_energy[...], (lanes, nvir)).T
    vir_pairs[...] = jnp.concatenate([column_energy] * (nvir // lanes), axis=1) + vir_energy[...]

    def remote(source, slot, target, columns=slice(None)):
        return pltpu.make_async_remote_copy(
            src_ref=source.at[:, :, columns],
            dst_ref=slots.at[slot, :, :, columns],
            send_sem=send_sems.at[slot],
            recv_sem=recv_sems.at[slot],
            device_id=(target, core),
            device_id_type=MESH,
        )

    def arrived(slot):
        pltpu.make_async_copy(slots.at[slot], slots.at[slot], recv_sems.at[slot]).wait()

    def join(orbital, at):
        half_block = own.at[pl.ds(orbital * share, share), :, mine]
        return pltpu.make_async_remote_copy(
            src_ref=half_block,
            dst_ref=half_block,
            send_sem=join_sems.at[0, at],
            recv_sem=join_sems.at[1, at],
            device_id=(me, other),
            device_id_type=MESH,
        )

    own_half = own.at[:, :, mine]
    pltpu.make_async_copy(own_half, own_half, spread_sems.at[1]).wait()
    join(other, 0).start()
    piece = own.at[pl.ds(core * share, share)]
    first = jnp.where(last == 1, below, above)
    second = jnp.where(last == 1, above, below)
    for columns in (mine, theirs):
        remote(piece, 1, beside, columns).start()
        remote(piece, 2, along, columns).start()
        remote(piece, 5 - last, first, columns).start()
        if columns is mine:
            join(core, 1).start()
            join(core, 0).wait_recv()
    remote(piece, 3, across).start()
    remote(piece, 4 + last, second).start()
    pltpu.make_async_copy(piece, slots.at[0], recv_sems.at[0]).start()
    beside_source, along_source = 4 + column, 4 + row
    beyond = jnp.where(row == 0, above, below)
    join(other, 1).wait_recv()

    for i in range(block):
        own_t[i] = own[i].T

    near, far = 4 + last, 5 - last

    def forward(source):
        @pl.when(beside_source == source)
        def _():
            remote(slots.at[source], 6, beside).start()

        @pl.when(along_source == source)
        def _():
            remote(slots.at[source], 7, along).start()

    def visit(step, carry):
        slot = jnp.where(step == 1, near, jnp.where(step == 4, far, jnp.where(step == 5, 3, step)))
        slot = jnp.where(step == 2, 1, jnp.where(step == 3, 2, slot))

        @pl.when(step != 5)
        def _():
            arrived(slot)

        @pl.when(step == 1)
        def _():
            forward(near)

        @pl.when(step == 4)
        def _():
            forward(far)
            arrived(3)
            remote(slots.at[3], 8, beyond).start()

        to_owner = jnp.where(slot == 0, me, jnp.where(slot == 1, beside, jnp.where(slot == 2, along, across)))
        from_beside = jnp.where(column == 1, beside + CYCLE, beside + aux_count - CYCLE)
        from_along = jnp.where(row == 1, along + CYCLE, along + aux_count - CYCLE)
        from_beyond = jnp.where(row == 1, across + CYCLE, across + aux_count - CYCLE)
        forwarded = jnp.where(slot == 6, from_beside, jnp.where(slot == 7, from_along, from_beyond))
        forwarded = lax.rem(forwarded, aux_count)
        stacked = jnp.where(slot == 4, above, below)
        owner = jnp.where(slot < 4, to_owner, jnp.where(slot < 6, stacked, forwarded))
        for s in range(share):
            pair_energy = occ_energy[owner * block + core * share + s]
            visitor = slots[slot, s]
            vis_t[...] = visitor.T
            for i in range(block):
                energy = occ_energy[me * block + i] + pair_energy
                for t in range(2):
                    rows = slice(t * half, (t + 1) * half)
                    direct = jnp.dot(own_t[i, rows], visitor, preferred_element_type=jnp.float32)
                    swapped = jnp.dot(vis_t[rows], own[i], preferred_element_type=jnp.float32)
                    inverse = 1.0 / (energy - vir_pairs[rows])
                    amp[i, rows] = (direct * inverse).astype(jnp.bfloat16)
                    mix[i, rows] = ((2.0 * direct - swapped) * inverse).astype(jnp.bfloat16)
                acc[i] += lax.dot_general(amp[i], mix[i], NT, preferred_element_type=jnp.float32)
        return carry

    lax.fori_loop(0, slot_count, visit, 0)

    outgoing[...] = acc[:, theirs].astype(bf16)
    swap = pltpu.make_async_remote_copy(
        src_ref=outgoing,
        dst_ref=incoming,
        send_sem=swap_sems.at[0],
        recv_sem=swap_sems.at[1],
        device_id=(me, other),
        device_id_type=MESH,
    )
    swap.start()
    for slot in range(1, slot_count):
        remote(piece, slot, beside).wait_send()
    for chunk in range(chunks):
        give(chunk).wait_send()
    join(other, 0).wait_send()
    join(core, 1).wait_send()
    sent = outbox.at[:, pl.ds(0, norb - block)]
    pltpu.make_async_copy(sent, sent, spread_sems.at[0]).wait()
    swap.wait()
    out_ref[...] = acc[:, mine] + incoming[...].astype(f32)


def shards(ints, occ_coef, vir_coef, occ_energy, vir_energy):
    aux_count = lax.axis_size("aux")
    ao_count = lax.axis_size("ao")
    held, part, nao = ints.shape
    norb, nvir = occ_coef.shape[1], vir_coef.shape[1]
    block, half, naux = norb // aux_count, nvir // ao_count, held * aux_count
    share = block // ao_count
    slot_count = 2 * CYCLE + 1
    groups, chunks = 4, 2
    depth = held // chunks
    f32, bf16 = jnp.float32, jnp.bfloat16
    anywhere = pl.BlockSpec(memory_space=pl.ANY)
    dma = pltpu.SemaphoreType.DMA
    return pl.pallas_call(
        functools.partial(density_kernel, aux_count, share),
        out_shape=jax.ShapeDtypeStruct((block, half, nvir), f32),
        in_specs=[anywhere] * 5,
        out_specs=pl.BlockSpec(memory_space=pltpu.VMEM),
        scratch_shapes=[
            pltpu.VMEM((groups, held // groups * part, nao), bf16),
            pltpu.VMEM((norb, nao), bf16),
            pltpu.VMEM((part, nvir), bf16),
            pltpu.SMEM((norb,), f32),
            pltpu.VMEM((1, nvir), f32),
            pltpu.VMEM((chunks, depth * norb, part), bf16),
            pltpu.VMEM((chunks, depth * norb, half), bf16),
            pltpu.VMEM((chunks, depth * norb, half), bf16),
            pltpu.VMEM((chunks, depth * norb, half), f32),
            pltpu.VMEM((chunks, norb, depth, half), bf16),
            pltpu.VMEM((block, naux, nvir), bf16),
            pltpu.VMEM((slot_count, share, naux, nvir), bf16),
            pltpu.VMEM((block, nvir, naux), bf16),
            pltpu.VMEM((nvir, naux), bf16),
            pltpu.VMEM((nvir, nvir), f32),
            pltpu.VMEM((block, nvir, nvir), bf16),
            pltpu.VMEM((block, nvir, nvir), bf16),
            pltpu.VMEM((block, nvir, nvir), f32),
            pltpu.VMEM((block, half, nvir), bf16),
            pltpu.VMEM((block, half, nvir), bf16),
            dma((groups,)),
            dma((4,)),
            dma((chunks,)),
            dma((chunks,)),
            dma((2,)),
            dma((2, 2)),
            dma((slot_count,)),
            dma((slot_count,)),
            dma((2,)),
        ],
        compiler_params=pltpu.CompilerParams(collective_id=0, has_side_effects=True, vmem_limit_bytes=60 * 2**20),
    )(ints.reshape(held * part, nao), occ_coef.T, vir_coef, occ_energy, vir_energy[None, :])


def solution(mesh):
    return jax.shard_map(
        shards,
        mesh=mesh,
        in_specs=(P("aux", "ao", None), P(), P("ao", None), P(), P()),
        out_specs=P("aux", "ao", None),
        check_vma=False,
    )
```

```python
import functools

import jax
import jax.numpy as jnp
from jax import lax
from jax.experimental import pallas as pl
from jax.experimental.pallas import tpu as pltpu
from jax.sharding import PartitionSpec as P

CYCLE = 4
MESH = pl.DeviceIdType.MESH
NT = (((1,), (1,)), ((), ()))


def places(me, aux_count):
    layers = aux_count // CYCLE
    layer, place = lax.div(me, CYCLE), lax.rem(me, CYCLE)
    column, row = lax.rem(place, 2), lax.div(place, 2)
    base = layer * CYCLE
    beside = base + place + 1 - 2 * column
    along = base + place + 2 - 4 * row
    across = base + CYCLE - 1 - place
    above = lax.rem(me + CYCLE, aux_count)
    below = lax.rem(me + aux_count - CYCLE, aux_count)
    last = jnp.where(layer == layers - 1, 1, 0)
    return column, row, beside, along, across, above, below, last


def density_kernel(
    aux_count, share, ints_ref, occ_ref, vir_ref, occ_energy_ref, vir_energy_ref, out_ref,
    ints, occ_t, vir, occ_energy, vir_energy, half_ints, given, taken, kept, outbox, own,
    slots, own_t, vis_t, vir_pairs, amp, mix, acc, outgoing, incoming,
    load_sems, input_sems, give_sems, take_sems, spread_sems, join_sems,
    send_sems, recv_sems, swap_sems,
):
    me = lax.axis_index("aux")
    core = lax.axis_index("ao")
    other = 1 - core
    block, naux, nvir = own.shape
    groups, rows_in_group, nao = ints.shape
    chunks, norb, depth, half = outbox.shape
    part = half_ints.shape[2]
    deep = naux // chunks
    slot_count = 2 * CYCLE + 1
    column, row, beside, along, across, above, below, last = places(me, aux_count)
    f32, bf16 = jnp.float32, jnp.bfloat16

    inputs = [
        pltpu.make_async_copy(source, target, input_sems.at[at])
        for at, (source, target) in enumerate(
            ((occ_ref, occ_t), (vir_ref, vir), (vir_energy_ref, vir_energy), (occ_energy_ref, occ_energy))
        )
    ]
    loads = [
        pltpu.make_async_copy(
            ints_ref.at[pl.ds(group * rows_in_group, rows_in_group)], ints.at[group], load_sems.at[group]
        )
        for group in range(groups)
    ]
    inputs[0].start()
    loads[0].start()
    for copy in inputs[1:] + loads[1:]:
        copy.start()

    barrier = pltpu.get_barrier_semaphore()

    def greet(step, carry):
        target = lax.rem(me + step, aux_count)
        pl.semaphore_signal(barrier, inc=1, device_id=(target, core), device_id_type=MESH)
        return carry

    lax.fori_loop(1, aux_count, greet, 0)
    pl.semaphore_signal(barrier, inc=1, device_id=(me, other), device_id_type=MESH)

    inputs[0].wait()
    occ = occ_t[...].T
    acc[...] = jnp.zeros_like(acc)
    inputs[1].wait()
    mine = pl.ds(pl.multiple_of(core * half, half), half)
    theirs = pl.ds(pl.multiple_of(other * half, half), half)
    to_row = lax.broadcasted_iota(jnp.int32, (norb * depth, norb * depth), 0)
    from_row = lax.broadcasted_iota(jnp.int32, (norb * depth, norb * depth), 1)
    order = jnp.where(from_row == lax.rem(to_row, depth) * norb + lax.div(to_row, depth), 1.0, 0.0).astype(bf16)

    def give(chunk):
        return pltpu.make_async_remote_copy(
            src_ref=given.at[chunk],
            dst_ref=taken.at[chunk],
            send_sem=give_sems.at[chunk],
            recv_sem=take_sems.at[chunk],
            device_id=(me, other),
            device_id_type=MESH,
        )

    def spread(chunk):
        give(chunk).wait_recv()
        total = kept[chunk] + taken[chunk].astype(f32)
        outbox[chunk] = total.astype(bf16).reshape(norb, depth, half)
        place = pl.ds(pl.multiple_of(chunk * deep + me * depth, depth), depth)

        def send(step, carry):
            target = lax.rem(me + step, aux_count)
            pltpu.make_async_remote_copy(
                src_ref=outbox.at[chunk, pl.ds(target * block, block)],
                dst_ref=own.at[:, place, mine],
                send_sem=spread_sems.at[chunks],
                recv_sem=spread_sems.at[chunk],
                device_id=(target, core),
                device_id_type=MESH,
            ).start()
            return carry

        lax.fori_loop(1, aux_count, send, 0)
        pltpu.make_async_copy(
            outbox.at[chunk, pl.ds(me * block, block)], own.at[:, place, mine], spread_sems.at[chunk]
        ).start()

    in_chunk = groups // chunks
    in_group = rows_in_group // part
    cut = rows_in_group // 2
    for group in range(groups):
        chunk = group // in_chunk
        loads[group].wait()
        for piece in range(2):
            product = jnp.dot(ints[group, piece * cut : (piece + 1) * cut], occ, preferred_element_type=f32).astype(bf16)
            for q in range(in_group // 2):
                at = ((group % in_chunk) * in_group + piece * (in_group // 2) + q) * norb
                half_ints[chunk, at : at + norb] = product[q * part : (q + 1) * part].T
        if group % in_chunk == in_chunk - 1:
            ordered = jnp.dot(order, half_ints[chunk], preferred_element_type=f32).astype(bf16)
            given[chunk] = jnp.dot(ordered, vir[:, theirs], preferred_element_type=f32).astype(bf16)
            if chunk == 0:
                pl.semaphore_wait(barrier, aux_count)
            give(chunk).start()
            kept[chunk] = jnp.dot(ordered, vir[:, mine], preferred_element_type=f32)
        elif chunk > 0:
            spread(chunk - 1)
    spread(chunks - 1)

    inputs[2].wait()
    inputs[3].wait()
    lanes = 128
    column_energy = jnp.broadcast_to(vir_energy[...], (lanes, nvir)).T
    vir_pairs[...] = jnp.concatenate([column_energy] * (nvir // lanes), axis=1) + vir_energy[...]

    def span(chunk):
        return pl.ds(chunk * deep, deep)

    def remote(source, slot, target, chunk, columns=slice(None)):
        return pltpu.make_async_remote_copy(
            src_ref=source.at[:, span(chunk), columns],
            dst_ref=slots.at[slot, :, span(chunk), columns],
            send_sem=send_sems.at[slot, chunk],
            recv_sem=recv_sems.at[slot, chunk],
            device_id=(target, core),
            device_id_type=MESH,
        )

    def arrived(slot, chunk):
        region = slots.at[slot, :, span(chunk)]
        pltpu.make_async_copy(region, region, recv_sems.at[slot, chunk]).wait()

    def join(orbital, at, chunk):
        half_block = own.at[pl.ds(orbital * share, share), span(chunk), mine]
        return pltpu.make_async_remote_copy(
            src_ref=half_block,
            dst_ref=half_block,
            send_sem=join_sems.at[0, at, chunk],
            recv_sem=join_sems.at[1, at, chunk],
            device_id=(me, other),
            device_id_type=MESH,
        )

    piece = own.at[pl.ds(core * share, share)]
    first = jnp.where(last == 1, below, above)
    second = jnp.where(last == 1, above, below)
    for chunk in range(chunks):
        own_half = own.at[:, span(chunk), mine]
        pltpu.make_async_copy(own_half, own_half, spread_sems.at[chunk]).wait()
        join(other, 0, chunk).start()
        for columns in (mine, theirs):
            remote(piece, 1, beside, chunk, columns).start()
            remote(piece, 2, along, chunk, columns).start()
            remote(piece, 5 - last, first, chunk, columns).start()
            if columns is mine:
                join(core, 1, chunk).start()
                join(core, 0, chunk).wait_recv()
        remote(piece, 3, across, chunk).start()
        remote(piece, 4 + last, second, chunk).start()
        pltpu.make_async_copy(
            piece.at[:, span(chunk)], slots.at[0, :, span(chunk)], recv_sems.at[0, chunk]
        ).start()
    beside_source, along_source = 4 + column, 4 + row
    beyond = jnp.where(row == 0, above, below)
    for chunk in range(chunks):
        join(other, 1, chunk).wait_recv()

    for i in range(block):
        own_t[i] = own[i].T

    near, far = 4 + last, 5 - last

    def forward(source, chunk):
        @pl.when(beside_source == source)
        def _():
            remote(slots.at[source], 6, beside, chunk).start()

        @pl.when(along_source == source)
        def _():
            remote(slots.at[source], 7, along, chunk).start()

    def visit(step, carry):
        slot = jnp.where(step == 3, near, jnp.where(step == 4, far, jnp.where(step == 5, 3, step)))

        @pl.when(step == 1)
        def _():
            arrived(near, 0)
            forward(near, 0)

        @pl.when(step == 2)
        def _():
            arrived(3, 0)
            remote(slots.at[3], 8, beyond, 0).start()
            arrived(far, 0)
            forward(far, 0)

        @pl.when(step == 3)
        def _():
            arrived(near, 1)
            forward(near, 1)

        @pl.when(step == 4)
        def _():
            arrived(3, 1)
            remote(slots.at[3], 8, beyond, 1).start()
            arrived(far, 1)
            forward(far, 1)

        @pl.when((step < 3) | (step > 5))
        def _():
            for chunk in range(chunks):
                arrived(slot, chunk)

        to_owner = jnp.where(slot == 0, me, jnp.where(slot == 1, beside, jnp.where(slot == 2, along, across)))
        from_beside = jnp.where(column == 1, beside + CYCLE, beside + aux_count - CYCLE)
        from_along = jnp.where(row == 1, along + CYCLE, along + aux_count - CYCLE)
        from_beyond = jnp.where(row == 1, across + CYCLE, across + aux_count - CYCLE)
        forwarded = jnp.where(slot == 6, from_beside, jnp.where(slot == 7, from_along, from_beyond))
        forwarded = lax.rem(forwarded, aux_count)
        stacked = jnp.where(slot == 4, above, below)
        owner = jnp.where(slot < 4, to_owner, jnp.where(slot < 6, stacked, forwarded))
        for s in range(share):
            pair_energy = occ_energy[owner * block + core * share + s]
            visitor = slots[slot, s]
            vis_t[...] = visitor.T
            for i in range(block):
                energy = occ_energy[me * block + i] + pair_energy
                for t in range(2):
                    rows = slice(t * half, (t + 1) * half)
                    direct = jnp.dot(own_t[i, rows], visitor, preferred_element_type=jnp.float32)
                    swapped = jnp.dot(vis_t[rows], own[i], preferred_element_type=jnp.float32)
                    inverse = 1.0 / (energy - vir_pairs[rows])
                    amp[i, rows] = (direct * inverse).astype(jnp.bfloat16)
                    mix[i, rows] = ((2.0 * direct - swapped) * inverse).astype(jnp.bfloat16)
                acc[i] += lax.dot_general(amp[i], mix[i], NT, preferred_element_type=jnp.float32)
        return carry

    lax.fori_loop(0, slot_count, visit, 0)

    outgoing[...] = acc[:, theirs].astype(bf16)
    swap = pltpu.make_async_remote_copy(
        src_ref=outgoing,
        dst_ref=incoming,
        send_sem=swap_sems.at[0],
        recv_sem=swap_sems.at[1],
        device_id=(me, other),
        device_id_type=MESH,
    )
    swap.start()
    for slot in range(1, slot_count):
        for chunk in range(chunks):
            remote(piece, slot, beside, chunk).wait_send()
    for chunk in range(chunks):
        give(chunk).wait_send()
        join(other, 0, chunk).wait_send()
        join(core, 1, chunk).wait_send()
    sent = outbox.at[:, pl.ds(0, norb - block)]
    pltpu.make_async_copy(sent, sent, spread_sems.at[chunks]).wait()
    swap.wait()
    out_ref[...] = acc[:, mine] + incoming[...].astype(f32)


def shards(ints, occ_coef, vir_coef, occ_energy, vir_energy):
    aux_count = lax.axis_size("aux")
    ao_count = lax.axis_size("ao")
    held, part, nao = ints.shape
    norb, nvir = occ_coef.shape[1], vir_coef.shape[1]
    block, half, naux = norb // aux_count, nvir // ao_count, held * aux_count
    share = block // ao_count
    slot_count = 2 * CYCLE + 1
    groups, chunks = 4, 2
    depth = held // chunks
    f32, bf16 = jnp.float32, jnp.bfloat16
    anywhere = pl.BlockSpec(memory_space=pl.ANY)
    dma = pltpu.SemaphoreType.DMA
    operands = (ints.reshape(held * part, nao), occ_coef.T, vir_coef, occ_energy, vir_energy[None, :])
    return pl.pallas_call(
        functools.partial(density_kernel, aux_count, share),
        out_shape=jax.ShapeDtypeStruct((block, half, nvir), f32),
        in_specs=[anywhere] * 5,
        out_specs=pl.BlockSpec(memory_space=pltpu.VMEM),
        scratch_shapes=[
            pltpu.VMEM((groups, held // groups * part, nao), bf16),
            pltpu.VMEM((norb, nao), bf16),
            pltpu.VMEM((part, nvir), bf16),
            pltpu.SMEM((norb,), f32),
            pltpu.VMEM((1, nvir), f32),
            pltpu.VMEM((chunks, depth * norb, part), bf16),
            pltpu.VMEM((chunks, depth * norb, half), bf16),
            pltpu.VMEM((chunks, depth * norb, half), bf16),
            pltpu.VMEM((chunks, depth * norb, half), f32),
            pltpu.VMEM((chunks, norb, depth, half), bf16),
            pltpu.VMEM((block, naux, nvir), bf16),
            pltpu.VMEM((slot_count, share, naux, nvir), bf16),
            pltpu.VMEM((block, nvir, naux), bf16),
            pltpu.VMEM((nvir, naux), bf16),
            pltpu.VMEM((nvir, nvir), f32),
            pltpu.VMEM((block, nvir, nvir), bf16),
            pltpu.VMEM((block, nvir, nvir), bf16),
            pltpu.VMEM((block, nvir, nvir), f32),
            pltpu.VMEM((block, half, nvir), bf16),
            pltpu.VMEM((block, half, nvir), bf16),
            dma((groups,)),
            dma((4,)),
            dma((chunks,)),
            dma((chunks,)),
            dma((chunks + 1,)),
            dma((2, 2, chunks)),
            dma((slot_count, chunks)),
            dma((slot_count, chunks)),
            dma((2,)),
        ],
        compiler_params=pltpu.CompilerParams(collective_id=0, has_side_effects=True, vmem_limit_bytes=44 * 2**20),
    )(*(pltpu.with_memory_space_constraint(operand, pltpu.HBM) for operand in operands))


def solution(mesh):
    return jax.shard_map(
        shards,
        mesh=mesh,
        in_specs=(P("aux", "ao", None), P(), P("ao", None), P(), P()),
        out_specs=P("aux", "ao", None),
        check_vma=False,
    )
```

```python
import functools

import jax
import jax.numpy as jnp
from jax import lax
from jax.experimental import pallas as pl
from jax.experimental.pallas import tpu as pltpu
from jax.sharding import PartitionSpec as P

CYCLE = 4
MESH = pl.DeviceIdType.MESH


def places(me, aux_count):
    layers = aux_count // CYCLE
    layer, place = lax.div(me, CYCLE), lax.rem(me, CYCLE)
    column, row = lax.rem(place, 2), lax.div(place, 2)
    base = layer * CYCLE
    beside = base + place + 1 - 2 * column
    along = base + place + 2 - 4 * row
    across = base + CYCLE - 1 - place
    above = lax.rem(me + CYCLE, aux_count)
    below = lax.rem(me + aux_count - CYCLE, aux_count)
    last = jnp.where(layer == layers - 1, 1, 0)
    return column, row, beside, along, across, above, below, last


def density_kernel(
    aux_count, share, ints_ref, occ_ref, vir_ref, occ_energy_ref, vir_energy_ref, out_ref,
    ints, occ_t, vir, occ_energy, vir_energy, half_ints, given, taken, kept, outbox, own,
    slots, own_t, vir_pairs, amp, mix, acc, outgoing, incoming,
    load_sems, input_sems, give_sems, take_sems, spread_sems, join_sems,
    send_sems, recv_sems, swap_sems,
):
    me = lax.axis_index("aux")
    core = lax.axis_index("ao")
    other = 1 - core
    block, naux, nvir = own.shape
    groups, rows_in_group, nao = ints.shape
    chunks, norb, depth, half = outbox.shape
    part = half_ints.shape[2]
    deep = naux // chunks
    slot_count = 2 * CYCLE + 1
    column, row, beside, along, across, above, below, last = places(me, aux_count)
    f32, bf16 = jnp.float32, jnp.bfloat16

    inputs = [
        pltpu.make_async_copy(source, target, input_sems.at[at])
        for at, (source, target) in enumerate(
            ((occ_ref, occ_t), (vir_ref, vir), (vir_energy_ref, vir_energy), (occ_energy_ref, occ_energy))
        )
    ]
    loads = [
        pltpu.make_async_copy(
            ints_ref.at[pl.ds(group * rows_in_group, rows_in_group)], ints.at[group], load_sems.at[group]
        )
        for group in range(groups)
    ]
    inputs[0].start()
    loads[0].start()
    for copy in inputs[1:] + loads[1:]:
        copy.start()

    barrier = pltpu.get_barrier_semaphore()

    def greet(step, carry):
        target = lax.rem(me + step, aux_count)
        pl.semaphore_signal(barrier, inc=1, device_id=(target, core), device_id_type=MESH)
        return carry

    lax.fori_loop(1, aux_count, greet, 0)
    pl.semaphore_signal(barrier, inc=1, device_id=(me, other), device_id_type=MESH)

    inputs[0].wait()
    occ = occ_t[...].T
    acc[...] = jnp.zeros_like(acc)
    amp[block - 1] = jnp.zeros_like(amp[block - 1])
    mix[block - 1] = jnp.zeros_like(mix[block - 1])
    inputs[1].wait()
    mine = pl.ds(pl.multiple_of(core * half, half), half)
    theirs = pl.ds(pl.multiple_of(other * half, half), half)
    to_row = lax.broadcasted_iota(jnp.int32, (norb * depth, norb * depth), 0)
    from_row = lax.broadcasted_iota(jnp.int32, (norb * depth, norb * depth), 1)
    order = jnp.where(from_row == lax.rem(to_row, depth) * norb + lax.div(to_row, depth), 1.0, 0.0).astype(bf16)

    def give(chunk):
        return pltpu.make_async_remote_copy(
            src_ref=given.at[chunk],
            dst_ref=taken.at[chunk],
            send_sem=give_sems.at[chunk],
            recv_sem=take_sems.at[chunk],
            device_id=(me, other),
            device_id_type=MESH,
        )

    def spread(chunk):
        give(chunk).wait_recv()
        total = kept[chunk] + taken[chunk].astype(f32)
        outbox[chunk] = total.astype(bf16).reshape(norb, depth, half)
        place = pl.ds(pl.multiple_of(chunk * deep + me * depth, depth), depth)

        def send(step, carry):
            target = lax.rem(me + step, aux_count)
            pltpu.make_async_remote_copy(
                src_ref=outbox.at[chunk, pl.ds(target * block, block)],
                dst_ref=own.at[:, place, mine],
                send_sem=spread_sems.at[chunks],
                recv_sem=spread_sems.at[chunk],
                device_id=(target, core),
                device_id_type=MESH,
            ).start()
            return carry

        lax.fori_loop(1, aux_count, send, 0)
        pltpu.make_async_copy(
            outbox.at[chunk, pl.ds(me * block, block)], own.at[:, place, mine], spread_sems.at[chunk]
        ).start()

    in_chunk = groups // chunks
    in_group = rows_in_group // part
    cut = rows_in_group // 2
    for group in range(groups):
        chunk = group // in_chunk
        loads[group].wait()
        for piece in range(2):
            product = jnp.dot(ints[group, piece * cut : (piece + 1) * cut], occ, preferred_element_type=f32).astype(bf16)
            for q in range(in_group // 2):
                at = ((group % in_chunk) * in_group + piece * (in_group // 2) + q) * norb
                half_ints[chunk, at : at + norb] = product[q * part : (q + 1) * part].T
        if group % in_chunk == in_chunk - 1:
            ordered = jnp.dot(order, half_ints[chunk], preferred_element_type=f32).astype(bf16)
            given[chunk] = jnp.dot(ordered, vir[:, theirs], preferred_element_type=f32).astype(bf16)
            if chunk == 0:
                pl.semaphore_wait(barrier, aux_count)
            give(chunk).start()
            kept[chunk] = jnp.dot(ordered, vir[:, mine], preferred_element_type=f32)
        elif chunk > 0 and group % in_chunk == 0:
            spread(chunk - 1)
    spread(chunks - 1)

    inputs[2].wait()
    inputs[3].wait()
    lanes = 128
    column_energy = jnp.broadcast_to(vir_energy[...], (lanes, nvir)).T
    vir_pairs[...] = jnp.concatenate([column_energy] * (nvir // lanes), axis=1) + vir_energy[...]

    def span(chunk):
        return pl.ds(chunk * deep, deep)

    def remote(source, slot, target, chunk, columns=slice(None)):
        return pltpu.make_async_remote_copy(
            src_ref=source.at[:, span(chunk), columns],
            dst_ref=slots.at[slot, :, span(chunk), columns],
            send_sem=send_sems.at[slot, chunk],
            recv_sem=recv_sems.at[slot, chunk],
            device_id=(target, core),
            device_id_type=MESH,
        )

    def arrived(slot, chunk):
        region = slots.at[slot, :, span(chunk)]
        pltpu.make_async_copy(region, region, recv_sems.at[slot, chunk]).wait()

    def join(orbital, at, chunk):
        half_block = own.at[pl.ds(orbital * share, share), span(chunk), mine]
        return pltpu.make_async_remote_copy(
            src_ref=half_block,
            dst_ref=half_block,
            send_sem=join_sems.at[0, at, chunk],
            recv_sem=join_sems.at[1, at, chunk],
            device_id=(me, other),
            device_id_type=MESH,
        )

    piece = own.at[pl.ds(core * share, share)]
    first = jnp.where(last == 1, below, above)
    second = jnp.where(last == 1, above, below)
    for chunk in range(chunks):
        own_half = own.at[:, span(chunk), mine]
        pltpu.make_async_copy(own_half, own_half, spread_sems.at[chunk]).wait()
        join(other, 0, chunk).start()
        for columns in (mine, theirs):
            remote(piece, 1, beside, chunk, columns).start()
            remote(piece, 2, along, chunk, columns).start()
            remote(piece, 5 - last, first, chunk, columns).start()
            if columns is mine:
                join(core, 1, chunk).start()
                join(core, 0, chunk).wait_recv()
        remote(piece, 3, across, chunk).start()
        remote(piece, 4 + last, second, chunk).start()
        pltpu.make_async_copy(
            piece.at[:, span(chunk)], slots.at[0, :, span(chunk)], recv_sems.at[0, chunk]
        ).start()
    beside_source, along_source = 4 + column, 4 + row
    beyond = jnp.where(row == 0, above, below)
    for chunk in range(chunks):
        join(other, 1, chunk).wait_recv()

    for i in range(block):
        own_t[i] = own[i].T

    near, far = 4 + last, 5 - last

    def forward(source, chunk):
        @pl.when(beside_source == source)
        def _():
            remote(slots.at[source], 6, beside, chunk).start()

        @pl.when(along_source == source)
        def _():
            remote(slots.at[source], 7, along, chunk).start()

    def settle(i, rows=slice(None)):
        acc[i, rows] += jnp.dot(amp[i, rows], mix[i], preferred_element_type=f32)

    def swap(i):
        return pltpu.make_async_remote_copy(
            src_ref=outgoing.at[i],
            dst_ref=incoming.at[i],
            send_sem=swap_sems.at[0, i],
            recv_sem=swap_sems.at[1, i],
            device_id=(me, other),
            device_id_type=MESH,
        )

    def hand_over(i):
        outgoing[i] = acc[i, theirs].astype(bf16)
        swap(i).start()

    tiles = [slice(0, half), slice(half, nvir)]

    def visit(step, final=False):
        slot = jnp.where(step == 3, near, jnp.where(step == 4, far, jnp.where(step == 5, 3, step)))

        @pl.when(step == 1)
        def _():
            arrived(near, 0)
            forward(near, 0)

        @pl.when(step == 2)
        def _():
            arrived(3, 0)
            remote(slots.at[3], 8, beyond, 0).start()
            arrived(far, 0)
            forward(far, 0)

        @pl.when(step == 3)
        def _():
            arrived(near, 1)
            forward(near, 1)

        @pl.when(step == 4)
        def _():
            arrived(3, 1)
            remote(slots.at[3], 8, beyond, 1).start()
            arrived(far, 1)
            forward(far, 1)

        @pl.when((step < 3) | (step > 5))
        def _():
            for chunk in range(chunks):
                arrived(slot, chunk)

        to_owner = jnp.where(slot == 0, me, jnp.where(slot == 1, beside, jnp.where(slot == 2, along, across)))
        from_beside = jnp.where(column == 1, beside + CYCLE, beside + aux_count - CYCLE)
        from_along = jnp.where(row == 1, along + CYCLE, along + aux_count - CYCLE)
        from_beyond = jnp.where(row == 1, across + CYCLE, across + aux_count - CYCLE)
        forwarded = jnp.where(slot == 6, from_beside, jnp.where(slot == 7, from_along, from_beyond))
        forwarded = lax.rem(forwarded, aux_count)
        stacked = jnp.where(slot == 4, above, below)
        owner = jnp.where(slot < 4, to_owner, jnp.where(slot < 6, stacked, forwarded))
        for s in range(share):
            pair_energy = occ_energy[owner * block + core * share + s]
            visitor = slots[slot, s]
            for i in range(block):
                energy = occ_energy[me * block + i] + pair_energy
                for rows in tiles:
                    direct = jnp.dot(own_t[i, rows], visitor, preferred_element_type=f32)
                    amp[i, rows] = (direct * (1.0 / (energy - vir_pairs[rows]))).astype(bf16)
                settle((i - 1) % block)
                if final and s == share - 1 and i > 0:
                    hand_over(i - 1)
                for rows in tiles:
                    mix[i, rows] = 2 * amp[i, :, rows].T - amp[i, rows]

    def step_of(step, carry):
        visit(step)
        return carry

    lax.fori_loop(0, slot_count - 1, step_of, 0)
    visit(slot_count - 1, final=True)
    settle(block - 1, theirs)
    hand_over(block - 1)
    settle(block - 1, mine)
    for slot in range(1, slot_count):
        for chunk in range(chunks):
            remote(piece, slot, beside, chunk).wait_send()
    for chunk in range(chunks):
        give(chunk).wait_send()
        join(other, 0, chunk).wait_send()
        join(core, 1, chunk).wait_send()
    sent = outbox.at[:, pl.ds(0, norb - block)]
    pltpu.make_async_copy(sent, sent, spread_sems.at[chunks]).wait()
    for i in range(block):
        swap(i).wait()
        out_ref[i] = acc[i, mine] + incoming[i].astype(f32)


def shards(ints, occ_coef, vir_coef, occ_energy, vir_energy):
    aux_count = lax.axis_size("aux")
    ao_count = lax.axis_size("ao")
    held, part, nao = ints.shape
    norb, nvir = occ_coef.shape[1], vir_coef.shape[1]
    block, half, naux = norb // aux_count, nvir // ao_count, held * aux_count
    share = block // ao_count
    slot_count = 2 * CYCLE + 1
    groups, chunks = 4, 2
    depth = held // chunks
    f32, bf16 = jnp.float32, jnp.bfloat16
    anywhere = pl.BlockSpec(memory_space=pl.ANY)
    dma = pltpu.SemaphoreType.DMA
    operands = (ints.reshape(held * part, nao), occ_coef.T, vir_coef, occ_energy, vir_energy[None, :])
    return pl.pallas_call(
        functools.partial(density_kernel, aux_count, share),
        out_shape=jax.ShapeDtypeStruct((block, half, nvir), f32),
        in_specs=[anywhere] * 5,
        out_specs=pl.BlockSpec(memory_space=pltpu.VMEM),
        scratch_shapes=[
            pltpu.VMEM((groups, held // groups * part, nao), bf16),
            pltpu.VMEM((norb, nao), bf16),
            pltpu.VMEM((part, nvir), bf16),
            pltpu.SMEM((norb,), f32),
            pltpu.VMEM((1, nvir), f32),
            pltpu.VMEM((chunks, depth * norb, part), bf16),
            pltpu.VMEM((chunks, depth * norb, half), bf16),
            pltpu.VMEM((chunks, depth * norb, half), bf16),
            pltpu.VMEM((chunks, depth * norb, half), f32),
            pltpu.VMEM((chunks, norb, depth, half), bf16),
            pltpu.VMEM((block, naux, nvir), bf16),
            pltpu.VMEM((slot_count, share, naux, nvir), bf16),
            pltpu.VMEM((block, nvir, naux), bf16),
            pltpu.VMEM((nvir, nvir), f32),
            pltpu.VMEM((block, nvir, nvir), bf16),
            pltpu.VMEM((block, nvir, nvir), bf16),
            pltpu.VMEM((block, nvir, nvir), f32),
            pltpu.VMEM((block, half, nvir), bf16),
            pltpu.VMEM((block, half, nvir), bf16),
            dma((groups,)),
            dma((4,)),
            dma((chunks,)),
            dma((chunks,)),
            dma((chunks + 1,)),
            dma((2, 2, chunks)),
            dma((slot_count, chunks)),
            dma((slot_count, chunks)),
            dma((2, block)),
        ],
        compiler_params=pltpu.CompilerParams(collective_id=0, has_side_effects=True, vmem_limit_bytes=44 * 2**20),
    )(*(pltpu.with_memory_space_constraint(operand, pltpu.HBM) for operand in operands))


def solution(mesh):
    return jax.shard_map(
        shards,
        mesh=mesh,
        in_specs=(P("aux", "ao", None), P(), P("ao", None), P(), P()),
        out_specs=P("aux", "ao", None),
        check_vma=False,
    )
```

```python
import functools

import jax
import jax.numpy as jnp
from jax import lax
from jax.experimental import pallas as pl
from jax.experimental.pallas import tpu as pltpu
from jax.sharding import PartitionSpec as P

CYCLE = 4
MESH = pl.DeviceIdType.MESH


def places(me, aux_count):
    layers = aux_count // CYCLE
    layer, place = lax.div(me, CYCLE), lax.rem(me, CYCLE)
    column, row = lax.rem(place, 2), lax.div(place, 2)
    base = layer * CYCLE
    beside = base + place + 1 - 2 * column
    along = base + place + 2 - 4 * row
    across = base + CYCLE - 1 - place
    above = lax.rem(me + CYCLE, aux_count)
    below = lax.rem(me + aux_count - CYCLE, aux_count)
    last = jnp.where(layer == layers - 1, 1, 0)
    bottom = jnp.where(layer == 0, 1, 0)
    return column, row, beside, along, across, above, below, bottom, last


def density_kernel(
    aux_count, share, ints_ref, occ_ref, vir_ref, occ_energy_ref, vir_energy_ref, out_ref,
    ints, occ_t, vir, occ_energy, vir_energy, half_ints, given, taken, kept, outbox, own,
    slots, own_t, vir_pairs, amp, mix, acc, outgoing, incoming,
    load_sems, input_sems, give_sems, take_sems, spread_sems, join_sems,
    send_sems, recv_sems, swap_sems,
):
    me = lax.axis_index("aux")
    core = lax.axis_index("ao")
    other = 1 - core
    block, naux, nvir = own.shape
    groups, rows_in_group, nao = ints.shape
    chunks, norb, depth, half = outbox.shape
    part = half_ints.shape[2]
    deep = naux // chunks
    slot_count = 2 * CYCLE + 1
    column, row, beside, along, across, above, below, bottom, last = places(me, aux_count)
    f32, bf16 = jnp.float32, jnp.bfloat16

    inputs = [
        pltpu.make_async_copy(source, target, input_sems.at[at])
        for at, (source, target) in enumerate(
            ((occ_ref, occ_t), (vir_ref, vir), (vir_energy_ref, vir_energy), (occ_energy_ref, occ_energy))
        )
    ]
    loads = [
        pltpu.make_async_copy(
            ints_ref.at[pl.ds(group * rows_in_group, rows_in_group)], ints.at[group], load_sems.at[group]
        )
        for group in range(groups)
    ]
    inputs[0].start()
    loads[0].start()
    for copy in inputs[1:] + loads[1:]:
        copy.start()

    barrier = pltpu.get_barrier_semaphore()

    def greet(step, carry):
        target = lax.rem(me + step, aux_count)
        pl.semaphore_signal(barrier, inc=1, device_id=(target, core), device_id_type=MESH)
        return carry

    lax.fori_loop(1, aux_count, greet, 0)
    pl.semaphore_signal(barrier, inc=1, device_id=(me, other), device_id_type=MESH)

    inputs[0].wait()
    occ = occ_t[...].T
    acc[...] = jnp.zeros_like(acc)
    amp[block - 1] = jnp.zeros_like(amp[block - 1])
    mix[block - 1] = jnp.zeros_like(mix[block - 1])
    inputs[1].wait()
    mine = pl.ds(pl.multiple_of(core * half, half), half)
    theirs = pl.ds(pl.multiple_of(other * half, half), half)
    to_row = lax.broadcasted_iota(jnp.int32, (norb * depth, norb * depth), 0)
    from_row = lax.broadcasted_iota(jnp.int32, (norb * depth, norb * depth), 1)
    order = jnp.where(from_row == lax.rem(to_row, depth) * norb + lax.div(to_row, depth), 1.0, 0.0).astype(bf16)

    def give(chunk):
        return pltpu.make_async_remote_copy(
            src_ref=given.at[chunk],
            dst_ref=taken.at[chunk],
            send_sem=give_sems.at[chunk],
            recv_sem=take_sems.at[chunk],
            device_id=(me, other),
            device_id_type=MESH,
        )

    def spread(chunk):
        give(chunk).wait_recv()
        total = kept[chunk] + taken[chunk].astype(f32)
        outbox[chunk] = total.astype(bf16).reshape(norb, depth, half)
        place = pl.ds(pl.multiple_of(chunk * deep + me * depth, depth), depth)

        def send(step, carry):
            target = lax.rem(me + step, aux_count)
            pltpu.make_async_remote_copy(
                src_ref=outbox.at[chunk, pl.ds(target * block, block)],
                dst_ref=own.at[:, place, mine],
                send_sem=spread_sems.at[chunks],
                recv_sem=spread_sems.at[chunk],
                device_id=(target, core),
                device_id_type=MESH,
            ).start()
            return carry

        lax.fori_loop(1, aux_count, send, 0)
        pltpu.make_async_copy(
            outbox.at[chunk, pl.ds(me * block, block)], own.at[:, place, mine], spread_sems.at[chunk]
        ).start()

    in_chunk = groups // chunks
    in_group = rows_in_group // part
    cut = rows_in_group // 2
    for group in range(groups):
        chunk = group // in_chunk
        loads[group].wait()
        for piece in range(2):
            product = jnp.dot(ints[group, piece * cut : (piece + 1) * cut], occ, preferred_element_type=f32).astype(bf16)
            for q in range(in_group // 2):
                at = ((group % in_chunk) * in_group + piece * (in_group // 2) + q) * norb
                half_ints[chunk, at : at + norb] = product[q * part : (q + 1) * part].T
        if group % in_chunk == in_chunk - 1:
            ordered = jnp.dot(order, half_ints[chunk], preferred_element_type=f32).astype(bf16)
            given[chunk] = jnp.dot(ordered, vir[:, theirs], preferred_element_type=f32).astype(bf16)
            if chunk == 0:
                pl.semaphore_wait(barrier, aux_count)
            give(chunk).start()
            kept[chunk] = jnp.dot(ordered, vir[:, mine], preferred_element_type=f32)
        elif chunk > 0 and group % in_chunk == 0:
            spread(chunk - 1)
    spread(chunks - 1)

    inputs[2].wait()
    inputs[3].wait()
    lanes = 128
    column_energy = jnp.broadcast_to(vir_energy[...], (lanes, nvir)).T
    vir_pairs[...] = jnp.concatenate([column_energy] * (nvir // lanes), axis=1) + vir_energy[...]

    def span(chunk):
        return pl.ds(chunk * deep, deep)

    def remote(source, slot, target, chunk, columns=slice(None)):
        return pltpu.make_async_remote_copy(
            src_ref=source.at[:, span(chunk), columns],
            dst_ref=slots.at[slot, :, span(chunk), columns],
            send_sem=send_sems.at[slot, chunk],
            recv_sem=recv_sems.at[slot, chunk],
            device_id=(target, core),
            device_id_type=MESH,
        )

    def arrived(slot, chunk):
        region = slots.at[slot, :, span(chunk)]
        pltpu.make_async_copy(region, region, recv_sems.at[slot, chunk]).wait()

    def join(orbital, at, chunk):
        half_block = own.at[pl.ds(orbital * share, share), span(chunk), mine]
        return pltpu.make_async_remote_copy(
            src_ref=half_block,
            dst_ref=half_block,
            send_sem=join_sems.at[0, at, chunk],
            recv_sem=join_sems.at[1, at, chunk],
            device_id=(me, other),
            device_id_type=MESH,
        )

    piece = own.at[pl.ds(core * share, share)]
    first = jnp.where(last == 1, above, below)
    second = jnp.where(last == 1, below, above)
    for chunk in range(chunks):
        own_half = own.at[:, span(chunk), mine]
        pltpu.make_async_copy(own_half, own_half, spread_sems.at[chunk]).wait()
        join(other, 0, chunk).start()
        for columns in (mine, theirs):
            remote(piece, 3, across, chunk, columns).start()
            remote(piece, 4 + last, first, chunk, columns).start()
            if columns is mine:
                join(core, 1, chunk).start()
                join(core, 0, chunk).wait_recv()
        remote(piece, 5 - last, second, chunk).start()
        if chunk == 0:
            remote(piece, 1, beside, chunk).start()
            remote(piece, 2, along, chunk).start()
        pltpu.make_async_copy(
            piece.at[:, span(chunk)], slots.at[0, :, span(chunk)], recv_sems.at[0, chunk]
        ).start()
    beside_source, along_source = 4 + column, 4 + row
    beyond = jnp.where(row == 0, above, below)
    for chunk in range(chunks):
        join(other, 1, chunk).wait_recv()

    for i in range(block):
        own_t[i] = own[i].T

    early, late = 4 + bottom, 5 - bottom

    def forward(source, chunk):
        @pl.when(beside_source == source)
        def _():
            remote(slots.at[source], 6, beside, chunk).start()

        @pl.when(along_source == source)
        def _():
            remote(slots.at[source], 7, along, chunk).start()

    def settle(i, rows=slice(None)):
        acc[i, rows] += jnp.dot(amp[i, rows], mix[i], preferred_element_type=f32)

    def swap(i):
        return pltpu.make_async_remote_copy(
            src_ref=outgoing.at[i],
            dst_ref=incoming.at[i],
            send_sem=swap_sems.at[0, i],
            recv_sem=swap_sems.at[1, i],
            device_id=(me, other),
            device_id_type=MESH,
        )

    def hand_over(i):
        outgoing[i] = acc[i, theirs].astype(bf16)
        swap(i).start()

    tiles = [slice(0, half), slice(half, nvir)]

    def visit(step, final=False):
        slot = jnp.where(step == 1, 3, jnp.where(step == 2, early, jnp.where(step == 3, late, step)))
        slot = jnp.where(step == 4, 1, jnp.where(step == 5, 2, slot))

        @pl.when(step == 1)
        def _():
            for chunk in range(chunks):
                arrived(3, chunk)
                remote(slots.at[3], 8, beyond, chunk).start()
                if chunk == 0:
                    arrived(early, 0)
                    forward(early, 0)
                    arrived(late, 0)
                    forward(late, 0)
                    remote(piece, 1, beside, 1).start()
                    remote(piece, 2, along, 1).start()

        @pl.when(step == 2)
        def _():
            arrived(early, 1)
            forward(early, 1)

        @pl.when(step == 3)
        def _():
            arrived(late, 1)
            forward(late, 1)

        @pl.when((step < 1) | (step > 3))
        def _():
            for chunk in range(chunks):
                arrived(slot, chunk)

        to_owner = jnp.where(slot == 0, me, jnp.where(slot == 1, beside, jnp.where(slot == 2, along, across)))
        from_beside = jnp.where(column == 1, beside + CYCLE, beside + aux_count - CYCLE)
        from_along = jnp.where(row == 1, along + CYCLE, along + aux_count - CYCLE)
        from_beyond = jnp.where(row == 1, across + CYCLE, across + aux_count - CYCLE)
        forwarded = jnp.where(slot == 6, from_beside, jnp.where(slot == 7, from_along, from_beyond))
        forwarded = lax.rem(forwarded, aux_count)
        stacked = jnp.where(slot == 4, above, below)
        owner = jnp.where(slot < 4, to_owner, jnp.where(slot < 6, stacked, forwarded))
        for s in range(share):
            pair_energy = occ_energy[owner * block + core * share + s]
            visitor = slots[slot, s]
            for i in range(block):
                energy = occ_energy[me * block + i] + pair_energy
                for rows in tiles:
                    direct = jnp.dot(own_t[i, rows], visitor, preferred_element_type=f32)
                    amp[i, rows] = (direct * (1.0 / (energy - vir_pairs[rows]))).astype(bf16)
                settle((i - 1) % block)
                if final and s == share - 1 and i > 0:
                    hand_over(i - 1)
                for rows in tiles:
                    mix[i, rows] = 2 * amp[i, :, rows].T - amp[i, rows]

    def step_of(step, carry):
        visit(step)
        return carry

    lax.fori_loop(0, slot_count - 1, step_of, 0)
    visit(slot_count - 1, final=True)
    settle(block - 1, theirs)
    hand_over(block - 1)
    settle(block - 1, mine)
    for slot in range(1, slot_count):
        for chunk in range(chunks):
            remote(piece, slot, beside, chunk).wait_send()
    for chunk in range(chunks):
        give(chunk).wait_send()
        join(other, 0, chunk).wait_send()
        join(core, 1, chunk).wait_send()
    sent = outbox.at[:, pl.ds(0, norb - block)]
    pltpu.make_async_copy(sent, sent, spread_sems.at[chunks]).wait()
    for i in range(block):
        swap(i).wait()
        out_ref[i] = acc[i, mine] + incoming[i].astype(f32)


def shards(ints, occ_coef, vir_coef, occ_energy, vir_energy):
    aux_count = lax.axis_size("aux")
    ao_count = lax.axis_size("ao")
    held, part, nao = ints.shape
    norb, nvir = occ_coef.shape[1], vir_coef.shape[1]
    block, half, naux = norb // aux_count, nvir // ao_count, held * aux_count
    share = block // ao_count
    slot_count = 2 * CYCLE + 1
    groups, chunks = 4, 2
    depth = held // chunks
    f32, bf16 = jnp.float32, jnp.bfloat16
    anywhere = pl.BlockSpec(memory_space=pl.ANY)
    dma = pltpu.SemaphoreType.DMA
    operands = (ints.reshape(held * part, nao), occ_coef.T, vir_coef, occ_energy, vir_energy[None, :])
    return pl.pallas_call(
        functools.partial(density_kernel, aux_count, share),
        out_shape=jax.ShapeDtypeStruct((block, half, nvir), f32),
        in_specs=[anywhere] * 5,
        out_specs=pl.BlockSpec(memory_space=pltpu.VMEM),
        scratch_shapes=[
            pltpu.VMEM((groups, held // groups * part, nao), bf16),
            pltpu.VMEM((norb, nao), bf16),
            pltpu.VMEM((part, nvir), bf16),
            pltpu.SMEM((norb,), f32),
            pltpu.VMEM((1, nvir), f32),
            pltpu.VMEM((chunks, depth * norb, part), bf16),
            pltpu.VMEM((chunks, depth * norb, half), bf16),
            pltpu.VMEM((chunks, depth * norb, half), bf16),
            pltpu.VMEM((chunks, depth * norb, half), f32),
            pltpu.VMEM((chunks, norb, depth, half), bf16),
            pltpu.VMEM((block, naux, nvir), bf16),
            pltpu.VMEM((slot_count, share, naux, nvir), bf16),
            pltpu.VMEM((block, nvir, naux), bf16),
            pltpu.VMEM((nvir, nvir), f32),
            pltpu.VMEM((block, nvir, nvir), bf16),
            pltpu.VMEM((block, nvir, nvir), bf16),
            pltpu.VMEM((block, nvir, nvir), f32),
            pltpu.VMEM((block, half, nvir), bf16),
            pltpu.VMEM((block, half, nvir), bf16),
            dma((groups,)),
            dma((4,)),
            dma((chunks,)),
            dma((chunks,)),
            dma((chunks + 1,)),
            dma((2, 2, chunks)),
            dma((slot_count, chunks)),
            dma((slot_count, chunks)),
            dma((2, block)),
        ],
        compiler_params=pltpu.CompilerParams(collective_id=0, has_side_effects=True, vmem_limit_bytes=44 * 2**20),
    )(*(pltpu.with_memory_space_constraint(operand, pltpu.HBM) for operand in operands))


def solution(mesh):
    return jax.shard_map(
        shards,
        mesh=mesh,
        in_specs=(P("aux", "ao", None), P(), P("ao", None), P(), P()),
        out_specs=P("aux", "ao", None),
        check_vma=False,
    )
```

```python
import functools

import jax
import jax.numpy as jnp
from jax import lax
from jax.experimental import pallas as pl
from jax.experimental.pallas import tpu as pltpu
from jax.sharding import PartitionSpec as P

CYCLE = 4
MESH = pl.DeviceIdType.MESH


def places(me, aux_count):
    layers = aux_count // CYCLE
    layer, place = lax.div(me, CYCLE), lax.rem(me, CYCLE)
    column, row = lax.rem(place, 2), lax.div(place, 2)
    base = layer * CYCLE
    beside = base + place + 1 - 2 * column
    along = base + place + 2 - 4 * row
    across = base + CYCLE - 1 - place
    above = lax.rem(me + CYCLE, aux_count)
    below = lax.rem(me + aux_count - CYCLE, aux_count)
    last = jnp.where(layer == layers - 1, 1, 0)
    bottom = jnp.where(layer == 0, 1, 0)
    return column, row, beside, along, across, above, below, bottom, last


def density_kernel(
    aux_count, share, ints_ref, occ_ref, vir_ref, occ_energy_ref, vir_energy_ref, kept_ref, incoming,
    ints, occ_t, vir, occ_energy, vir_energy, half_ints, given, taken, kept, outbox, own,
    slots, own_t, vir_pairs, amp, mix, acc, outgoing,
    load_sems, input_sems, give_sems, take_sems, spread_sems, join_sems,
    send_sems, recv_sems, swap_sems,
):
    me = lax.axis_index("aux")
    core = lax.axis_index("ao")
    other = 1 - core
    block, naux, nvir = own.shape
    groups, rows_in_group, nao = ints.shape
    chunks, norb, depth, half = outbox.shape
    part = half_ints.shape[2]
    deep = naux // chunks
    slot_count = 2 * CYCLE + 1
    column, row, beside, along, across, above, below, bottom, last = places(me, aux_count)
    f32, bf16 = jnp.float32, jnp.bfloat16

    inputs = [
        pltpu.make_async_copy(source, target, input_sems.at[at])
        for at, (source, target) in enumerate(
            ((occ_ref, occ_t), (vir_ref, vir), (vir_energy_ref, vir_energy), (occ_energy_ref, occ_energy))
        )
    ]
    loads = [
        pltpu.make_async_copy(
            ints_ref.at[pl.ds(group * rows_in_group, rows_in_group)], ints.at[group], load_sems.at[group]
        )
        for group in range(groups)
    ]
    inputs[0].start()
    loads[0].start()
    for copy in inputs[1:] + loads[1:]:
        copy.start()

    barrier = pltpu.get_barrier_semaphore()

    def greet(step, carry):
        target = lax.rem(me + step, aux_count)
        pl.semaphore_signal(barrier, inc=1, device_id=(target, core), device_id_type=MESH)
        return carry

    lax.fori_loop(1, aux_count, greet, 0)
    pl.semaphore_signal(barrier, inc=1, device_id=(me, other), device_id_type=MESH)

    inputs[0].wait()
    occ = occ_t[...].T
    acc[...] = jnp.zeros_like(acc)
    amp[block - 1] = jnp.zeros_like(amp[block - 1])
    mix[block - 1] = jnp.zeros_like(mix[block - 1])
    inputs[1].wait()
    mine = pl.ds(pl.multiple_of(core * half, half), half)
    theirs = pl.ds(pl.multiple_of(other * half, half), half)
    to_row = lax.broadcasted_iota(jnp.int32, (norb * depth, norb * depth), 0)
    from_row = lax.broadcasted_iota(jnp.int32, (norb * depth, norb * depth), 1)
    order = jnp.where(from_row == lax.rem(to_row, depth) * norb + lax.div(to_row, depth), 1.0, 0.0).astype(bf16)

    def give(chunk):
        return pltpu.make_async_remote_copy(
            src_ref=given.at[chunk],
            dst_ref=taken.at[chunk],
            send_sem=give_sems.at[chunk],
            recv_sem=take_sems.at[chunk],
            device_id=(me, other),
            device_id_type=MESH,
        )

    def spread(chunk):
        give(chunk).wait_recv()
        total = kept[chunk] + taken[chunk].astype(f32)
        outbox[chunk] = total.astype(bf16).reshape(norb, depth, half)
        place = pl.ds(pl.multiple_of(chunk * deep + me * depth, depth), depth)

        def send(step, carry):
            target = lax.rem(me + step, aux_count)
            pltpu.make_async_remote_copy(
                src_ref=outbox.at[chunk, pl.ds(target * block, block)],
                dst_ref=own.at[:, place, mine],
                send_sem=spread_sems.at[chunks],
                recv_sem=spread_sems.at[chunk],
                device_id=(target, core),
                device_id_type=MESH,
            ).start()
            return carry

        lax.fori_loop(1, aux_count, send, 0)
        pltpu.make_async_copy(
            outbox.at[chunk, pl.ds(me * block, block)], own.at[:, place, mine], spread_sems.at[chunk]
        ).start()

    in_chunk = groups // chunks
    in_group = rows_in_group // part
    cut = rows_in_group // 2
    for group in range(groups):
        chunk = group // in_chunk
        loads[group].wait()
        for piece in range(2):
            product = jnp.dot(ints[group, piece * cut : (piece + 1) * cut], occ, preferred_element_type=f32).astype(bf16)
            for q in range(in_group // 2):
                at = ((group % in_chunk) * in_group + piece * (in_group // 2) + q) * norb
                half_ints[chunk, at : at + norb] = product[q * part : (q + 1) * part].T
        if group % in_chunk == in_chunk - 1:
            ordered = jnp.dot(order, half_ints[chunk], preferred_element_type=f32).astype(bf16)
            given[chunk] = jnp.dot(ordered, vir[:, theirs], preferred_element_type=f32).astype(bf16)
            if chunk == 0:
                pl.semaphore_wait(barrier, aux_count)
            give(chunk).start()
            kept[chunk] = jnp.dot(ordered, vir[:, mine], preferred_element_type=f32)
        elif chunk > 0 and group % in_chunk == 0:
            spread(chunk - 1)
    spread(chunks - 1)

    inputs[2].wait()
    inputs[3].wait()
    lanes = 128
    column_energy = jnp.broadcast_to(vir_energy[...], (lanes, nvir)).T
    vir_pairs[...] = jnp.concatenate([column_energy] * (nvir // lanes), axis=1) + vir_energy[...]

    def span(chunk):
        return pl.ds(chunk * deep, deep)

    def remote(source, slot, target, chunk, columns=slice(None)):
        return pltpu.make_async_remote_copy(
            src_ref=source.at[:, span(chunk), columns],
            dst_ref=slots.at[slot, :, span(chunk), columns],
            send_sem=send_sems.at[slot, chunk],
            recv_sem=recv_sems.at[slot, chunk],
            device_id=(target, core),
            device_id_type=MESH,
        )

    def arrived(slot, chunk):
        region = slots.at[slot, :, span(chunk)]
        pltpu.make_async_copy(region, region, recv_sems.at[slot, chunk]).wait()

    def join(orbital, at, chunk):
        half_block = own.at[pl.ds(orbital * share, share), span(chunk), mine]
        return pltpu.make_async_remote_copy(
            src_ref=half_block,
            dst_ref=half_block,
            send_sem=join_sems.at[0, at, chunk],
            recv_sem=join_sems.at[1, at, chunk],
            device_id=(me, other),
            device_id_type=MESH,
        )

    piece = own.at[pl.ds(core * share, share)]
    first = jnp.where(last == 1, above, below)
    second = jnp.where(last == 1, below, above)
    for chunk in range(chunks):
        own_half = own.at[:, span(chunk), mine]
        pltpu.make_async_copy(own_half, own_half, spread_sems.at[chunk]).wait()
        join(other, 0, chunk).start()
        for columns in (mine, theirs):
            remote(piece, 3, across, chunk, columns).start()
            remote(piece, 4 + last, first, chunk, columns).start()
            if columns is mine:
                join(core, 1, chunk).start()
                join(core, 0, chunk).wait_recv()
        remote(piece, 5 - last, second, chunk).start()
        if chunk == 0:
            remote(piece, 1, beside, chunk).start()
            remote(piece, 2, along, chunk).start()
        pltpu.make_async_copy(
            piece.at[:, span(chunk)], slots.at[0, :, span(chunk)], recv_sems.at[0, chunk]
        ).start()
    beside_source, along_source = 4 + column, 4 + row
    beyond = jnp.where(row == 0, above, below)
    for chunk in range(chunks):
        join(other, 1, chunk).wait_recv()

    for i in range(block):
        own_t[i] = own[i].T

    early, late = 4 + bottom, 5 - bottom

    def forward(source, chunk):
        @pl.when(beside_source == source)
        def _():
            remote(slots.at[source], 6, beside, chunk).start()

        @pl.when(along_source == source)
        def _():
            remote(slots.at[source], 7, along, chunk).start()

    def settle(i, rows=slice(None)):
        acc[i, rows] += jnp.dot(amp[i, rows], mix[i], preferred_element_type=f32)

    def swap(i):
        return pltpu.make_async_remote_copy(
            src_ref=outgoing.at[i],
            dst_ref=incoming.at[i],
            send_sem=swap_sems.at[0, i],
            recv_sem=swap_sems.at[1, i],
            device_id=(me, other),
            device_id_type=MESH,
        )

    def hand_over(i):
        outgoing[i] = acc[i, theirs].astype(bf16)
        swap(i).start()

    tiles = [slice(0, half), slice(half, nvir)]

    def visit(step, final=False):
        slot = jnp.where(step == 1, 3, jnp.where(step == 2, early, jnp.where(step == 3, late, step)))
        slot = jnp.where(step == 4, 1, jnp.where(step == 5, 2, slot))

        @pl.when(step == 1)
        def _():
            for chunk in range(chunks):
                arrived(3, chunk)
                remote(slots.at[3], 8, beyond, chunk).start()
                if chunk == 0:
                    arrived(early, 0)
                    forward(early, 0)
                    arrived(late, 0)
                    forward(late, 0)
                    remote(piece, 1, beside, 1).start()
                    remote(piece, 2, along, 1).start()

        @pl.when(step == 2)
        def _():
            arrived(early, 1)
            forward(early, 1)

        @pl.when(step == 3)
        def _():
            arrived(late, 1)
            forward(late, 1)

        @pl.when((step < 1) | (step > 3))
        def _():
            for chunk in range(chunks):
                arrived(slot, chunk)

        to_owner = jnp.where(slot == 0, me, jnp.where(slot == 1, beside, jnp.where(slot == 2, along, across)))
        from_beside = jnp.where(column == 1, beside + CYCLE, beside + aux_count - CYCLE)
        from_along = jnp.where(row == 1, along + CYCLE, along + aux_count - CYCLE)
        from_beyond = jnp.where(row == 1, across + CYCLE, across + aux_count - CYCLE)
        forwarded = jnp.where(slot == 6, from_beside, jnp.where(slot == 7, from_along, from_beyond))
        forwarded = lax.rem(forwarded, aux_count)
        stacked = jnp.where(slot == 4, above, below)
        owner = jnp.where(slot < 4, to_owner, jnp.where(slot < 6, stacked, forwarded))
        for s in range(share):
            pair_energy = occ_energy[owner * block + core * share + s]
            visitor = slots[slot, s]
            for i in range(block):
                energy = occ_energy[me * block + i] + pair_energy
                for rows in tiles:
                    direct = jnp.dot(own_t[i, rows], visitor, preferred_element_type=f32)
                    amp[i, rows] = (direct * (1.0 / (energy - vir_pairs[rows]))).astype(bf16)
                settle((i - 1) % block)
                if final and s == share - 1 and i > 0:
                    hand_over(i - 1)
                for rows in tiles:
                    mix[i, rows] = 2 * amp[i, :, rows].T - amp[i, rows]

    def step_of(step, carry):
        visit(step)
        return carry

    lax.fori_loop(0, slot_count - 1, step_of, 0)
    visit(slot_count - 1, final=True)
    settle(block - 1, theirs)
    hand_over(block - 1)
    settle(block - 1, mine)
    for slot in range(1, slot_count):
        for chunk in range(chunks):
            remote(piece, slot, beside, chunk).wait_send()
    for chunk in range(chunks):
        give(chunk).wait_send()
        join(other, 0, chunk).wait_send()
        join(core, 1, chunk).wait_send()
    sent = outbox.at[:, pl.ds(0, norb - block)]
    pltpu.make_async_copy(sent, sent, spread_sems.at[chunks]).wait()
    for i in range(block):
        kept_ref[i] = acc[i, mine]
    for i in range(block):
        swap(i).wait()


def shards(ints, occ_coef, vir_coef, occ_energy, vir_energy):
    aux_count = lax.axis_size("aux")
    ao_count = lax.axis_size("ao")
    held, part, nao = ints.shape
    norb, nvir = occ_coef.shape[1], vir_coef.shape[1]
    block, half, naux = norb // aux_count, nvir // ao_count, held * aux_count
    share = block // ao_count
    slot_count = 2 * CYCLE + 1
    groups, chunks = 4, 2
    depth = held // chunks
    f32, bf16 = jnp.float32, jnp.bfloat16
    anywhere = pl.BlockSpec(memory_space=pl.ANY)
    dma = pltpu.SemaphoreType.DMA
    operands = (ints.reshape(held * part, nao), occ_coef.T, vir_coef, occ_energy, vir_energy[None, :])
    kept, incoming = pl.pallas_call(
        functools.partial(density_kernel, aux_count, share),
        out_shape=[jax.ShapeDtypeStruct((block, half, nvir), kind) for kind in (f32, bf16)],
        in_specs=[anywhere] * 5,
        out_specs=[pl.BlockSpec(memory_space=pltpu.VMEM)] * 2,
        scratch_shapes=[
            pltpu.VMEM((groups, held // groups * part, nao), bf16),
            pltpu.VMEM((norb, nao), bf16),
            pltpu.VMEM((part, nvir), bf16),
            pltpu.SMEM((norb,), f32),
            pltpu.VMEM((1, nvir), f32),
            pltpu.VMEM((chunks, depth * norb, part), bf16),
            pltpu.VMEM((chunks, depth * norb, half), bf16),
            pltpu.VMEM((chunks, depth * norb, half), bf16),
            pltpu.VMEM((chunks, depth * norb, half), f32),
            pltpu.VMEM((chunks, norb, depth, half), bf16),
            pltpu.VMEM((block, naux, nvir), bf16),
            pltpu.VMEM((slot_count, share, naux, nvir), bf16),
            pltpu.VMEM((block, nvir, naux), bf16),
            pltpu.VMEM((nvir, nvir), f32),
            pltpu.VMEM((block, nvir, nvir), bf16),
            pltpu.VMEM((block, nvir, nvir), bf16),
            pltpu.VMEM((block, nvir, nvir), f32),
            pltpu.VMEM((block, half, nvir), bf16),
            dma((groups,)),
            dma((4,)),
            dma((chunks,)),
            dma((chunks,)),
            dma((chunks + 1,)),
            dma((2, 2, chunks)),
            dma((slot_count, chunks)),
            dma((slot_count, chunks)),
            dma((2, block)),
        ],
        compiler_params=pltpu.CompilerParams(collective_id=0, has_side_effects=True, vmem_limit_bytes=44 * 2**20),
    )(*(pltpu.with_memory_space_constraint(operand, pltpu.HBM) for operand in operands))
    return kept + incoming.astype(f32)


def solution(mesh):
    return jax.shard_map(
        shards,
        mesh=mesh,
        in_specs=(P("aux", "ao", None), P(), P("ao", None), P(), P()),
        out_specs=P("aux", "ao", None),
        check_vma=False,
    )
```

```python
import functools

import jax
import jax.numpy as jnp
from jax import lax
from jax.experimental import pallas as pl
from jax.experimental.pallas import tpu as pltpu
from jax.sharding import PartitionSpec as P

CYCLE = 4
MESH = pl.DeviceIdType.MESH


def places(me, aux_count):
    layers = aux_count // CYCLE
    layer, place = lax.div(me, CYCLE), lax.rem(me, CYCLE)
    column, row = lax.rem(place, 2), lax.div(place, 2)
    base = layer * CYCLE
    beside = base + place + 1 - 2 * column
    along = base + place + 2 - 4 * row
    across = base + CYCLE - 1 - place
    above = lax.rem(me + CYCLE, aux_count)
    below = lax.rem(me + aux_count - CYCLE, aux_count)
    last = jnp.where(layer == layers - 1, 1, 0)
    bottom = jnp.where(layer == 0, 1, 0)
    return column, row, beside, along, across, above, below, bottom, last


def density_kernel(
    aux_count, share, ints_ref, occ_ref, vir_ref, occ_energy_ref, vir_energy_ref, out_ref,
    ints, occ_t, vir, occ_energy, vir_energy, half_ints, given, taken, kept, outbox, own,
    slots, own_t, vir_pairs, amp, mix, acc, outgoing, incoming,
    load_sems, input_sems, give_sems, take_sems, spread_sems, join_sems,
    send_sems, recv_sems, swap_sems,
):
    me = lax.axis_index("aux")
    core = lax.axis_index("ao")
    other = 1 - core
    block, naux, nvir = own.shape
    groups, rows_in_group, nao = ints.shape
    chunks, norb, depth, half = outbox.shape
    part = half_ints.shape[2]
    deep = naux // chunks
    slot_count = 2 * CYCLE + 1
    column, row, beside, along, across, above, below, bottom, last = places(me, aux_count)
    f32, bf16 = jnp.float32, jnp.bfloat16

    inputs = [
        pltpu.make_async_copy(source, target, input_sems.at[at])
        for at, (source, target) in enumerate(
            ((occ_ref, occ_t), (vir_ref, vir), (vir_energy_ref, vir_energy), (occ_energy_ref, occ_energy))
        )
    ]
    loads = [
        pltpu.make_async_copy(
            ints_ref.at[pl.ds(group * rows_in_group, rows_in_group)], ints.at[group], load_sems.at[group]
        )
        for group in range(groups)
    ]
    inputs[0].start()
    loads[0].start()
    for copy in inputs[1:] + loads[1:]:
        copy.start()

    barrier = pltpu.get_barrier_semaphore()

    def greet(step, carry):
        target = lax.rem(me + step, aux_count)
        pl.semaphore_signal(barrier, inc=1, device_id=(target, core), device_id_type=MESH)
        return carry

    lax.fori_loop(1, aux_count, greet, 0)
    pl.semaphore_signal(barrier, inc=1, device_id=(me, other), device_id_type=MESH)

    inputs[0].wait()
    occ = occ_t[...].T
    acc[...] = jnp.zeros_like(acc)
    amp[block - 1] = jnp.zeros_like(amp[block - 1])
    mix[block - 1] = jnp.zeros_like(mix[block - 1])
    inputs[1].wait()
    mine = pl.ds(pl.multiple_of(core * half, half), half)
    theirs = pl.ds(pl.multiple_of(other * half, half), half)
    to_row = lax.broadcasted_iota(jnp.int32, (norb * depth, norb * depth), 0)
    from_row = lax.broadcasted_iota(jnp.int32, (norb * depth, norb * depth), 1)
    order = jnp.where(from_row == lax.rem(to_row, depth) * norb + lax.div(to_row, depth), 1.0, 0.0).astype(bf16)

    def give(chunk):
        return pltpu.make_async_remote_copy(
            src_ref=given.at[chunk],
            dst_ref=taken.at[chunk],
            send_sem=give_sems.at[chunk],
            recv_sem=take_sems.at[chunk],
            device_id=(me, other),
            device_id_type=MESH,
        )

    def spread(chunk):
        give(chunk).wait_recv()
        total = kept[chunk] + taken[chunk].astype(f32)
        outbox[chunk] = total.astype(bf16).reshape(norb, depth, half)
        place = pl.ds(pl.multiple_of(chunk * deep + me * depth, depth), depth)

        def send(step, carry):
            target = lax.rem(me + step, aux_count)
            pltpu.make_async_remote_copy(
                src_ref=outbox.at[chunk, pl.ds(target * block, block)],
                dst_ref=own.at[:, place, mine],
                send_sem=spread_sems.at[chunks],
                recv_sem=spread_sems.at[chunk],
                device_id=(target, core),
                device_id_type=MESH,
            ).start()
            return carry

        lax.fori_loop(1, aux_count, send, 0)
        pltpu.make_async_copy(
            outbox.at[chunk, pl.ds(me * block, block)], own.at[:, place, mine], spread_sems.at[chunk]
        ).start()

    in_chunk = groups // chunks
    in_group = rows_in_group // part
    cut = rows_in_group // 2
    for group in range(groups):
        chunk = group // in_chunk
        loads[group].wait()
        for piece in range(2):
            product = jnp.dot(ints[group, piece * cut : (piece + 1) * cut], occ, preferred_element_type=f32).astype(bf16)
            for q in range(in_group // 2):
                at = ((group % in_chunk) * in_group + piece * (in_group // 2) + q) * norb
                half_ints[chunk, at : at + norb] = product[q * part : (q + 1) * part].T
        if group % in_chunk == in_chunk - 1:
            ordered = jnp.dot(order, half_ints[chunk], preferred_element_type=f32).astype(bf16)
            given[chunk] = jnp.dot(ordered, vir[:, theirs], preferred_element_type=f32).astype(bf16)
            if chunk == 0:
                pl.semaphore_wait(barrier, aux_count)
            give(chunk).start()
            kept[chunk] = jnp.dot(ordered, vir[:, mine], preferred_element_type=f32)
        elif chunk > 0 and group % in_chunk == 0:
            spread(chunk - 1)
    spread(chunks - 1)

    inputs[2].wait()
    inputs[3].wait()
    lanes = 128
    column_energy = jnp.broadcast_to(vir_energy[...], (lanes, nvir)).T
    vir_pairs[...] = jnp.concatenate([column_energy] * (nvir // lanes), axis=1) + vir_energy[...]

    def span(chunk):
        return pl.ds(chunk * deep, deep)

    def remote(source, slot, target, chunk, columns=slice(None)):
        return pltpu.make_async_remote_copy(
            src_ref=source.at[:, span(chunk), columns],
            dst_ref=slots.at[slot, :, span(chunk), columns],
            send_sem=send_sems.at[slot, chunk],
            recv_sem=recv_sems.at[slot, chunk],
            device_id=(target, core),
            device_id_type=MESH,
        )

    def arrived(slot, chunk):
        region = slots.at[slot, :, span(chunk)]
        pltpu.make_async_copy(region, region, recv_sems.at[slot, chunk]).wait()

    def join(orbital, at, chunk):
        half_block = own.at[pl.ds(orbital * share, share), span(chunk), mine]
        return pltpu.make_async_remote_copy(
            src_ref=half_block,
            dst_ref=half_block,
            send_sem=join_sems.at[0, at, chunk],
            recv_sem=join_sems.at[1, at, chunk],
            device_id=(me, other),
            device_id_type=MESH,
        )

    piece = own.at[pl.ds(core * share, share)]
    first = jnp.where(last == 1, above, below)
    second = jnp.where(last == 1, below, above)
    for chunk in range(chunks):
        own_half = own.at[:, span(chunk), mine]
        pltpu.make_async_copy(own_half, own_half, spread_sems.at[chunk]).wait()
        join(other, 0, chunk).start()
        for columns in (mine, theirs):
            remote(piece, 3, across, chunk, columns).start()
            remote(piece, 4 + last, first, chunk, columns).start()
            if columns is mine:
                join(core, 1, chunk).start()
                join(core, 0, chunk).wait_recv()
        remote(piece, 5 - last, second, chunk).start()
        if chunk == 0:
            remote(piece, 1, beside, chunk).start()
            remote(piece, 2, along, chunk).start()
        pltpu.make_async_copy(
            piece.at[:, span(chunk)], slots.at[0, :, span(chunk)], recv_sems.at[0, chunk]
        ).start()
    beside_source, along_source = 4 + column, 4 + row
    beyond = jnp.where(row == 0, above, below)
    for chunk in range(chunks):
        join(other, 1, chunk).wait_recv()

    for i in range(block):
        own_t[i] = own[i].T

    early, late = 4 + bottom, 5 - bottom

    def forward(source, chunk):
        @pl.when(beside_source == source)
        def _():
            remote(slots.at[source], 6, beside, chunk).start()

        @pl.when(along_source == source)
        def _():
            remote(slots.at[source], 7, along, chunk).start()

    def settle(i, rows=slice(None)):
        acc[i, rows] += jnp.dot(amp[i, rows], mix[i], preferred_element_type=f32)

    def swap(i):
        return pltpu.make_async_remote_copy(
            src_ref=outgoing.at[i],
            dst_ref=incoming.at[i],
            send_sem=swap_sems.at[0, i],
            recv_sem=swap_sems.at[1, i],
            device_id=(me, other),
            device_id_type=MESH,
        )

    def hand_over(i):
        outgoing[i] = acc[i, theirs].astype(bf16)
        swap(i).start()

    tiles = [slice(0, nvir)]

    def visit(step, final=False):
        slot = jnp.where(step == 1, 3, jnp.where(step == 2, early, jnp.where(step == 3, late, step)))
        slot = jnp.where(step == 4, 1, jnp.where(step == 5, 2, slot))

        @pl.when(step == 1)
        def _():
            for chunk in range(chunks):
                arrived(3, chunk)
                remote(slots.at[3], 8, beyond, chunk).start()
                if chunk == 0:
                    arrived(early, 0)
                    forward(early, 0)
                    arrived(late, 0)
                    forward(late, 0)
                    remote(piece, 1, beside, 1).start()
                    remote(piece, 2, along, 1).start()

        @pl.when(step == 2)
        def _():
            arrived(early, 1)
            forward(early, 1)

        @pl.when(step == 3)
        def _():
            arrived(late, 1)
            forward(late, 1)

        @pl.when((step < 1) | (step > 3))
        def _():
            for chunk in range(chunks):
                arrived(slot, chunk)

        to_owner = jnp.where(slot == 0, me, jnp.where(slot == 1, beside, jnp.where(slot == 2, along, across)))
        from_beside = jnp.where(column == 1, beside + CYCLE, beside + aux_count - CYCLE)
        from_along = jnp.where(row == 1, along + CYCLE, along + aux_count - CYCLE)
        from_beyond = jnp.where(row == 1, across + CYCLE, across + aux_count - CYCLE)
        forwarded = jnp.where(slot == 6, from_beside, jnp.where(slot == 7, from_along, from_beyond))
        forwarded = lax.rem(forwarded, aux_count)
        stacked = jnp.where(slot == 4, above, below)
        owner = jnp.where(slot < 4, to_owner, jnp.where(slot < 6, stacked, forwarded))
        for s in range(share):
            pair_energy = occ_energy[owner * block + core * share + s]
            visitor = slots[slot, s]
            for i in range(block):
                energy = occ_energy[me * block + i] + pair_energy
                for rows in tiles:
                    direct = jnp.dot(own_t[i, rows], visitor, preferred_element_type=f32)
                    amp[i, rows] = (direct * (1.0 / (energy - vir_pairs[rows]))).astype(bf16)
                settle((i - 1) % block)
                if final and s == share - 1 and i > 0:
                    hand_over(i - 1)
                for rows in tiles:
                    mix[i, rows] = 2 * amp[i, :, rows].T - amp[i, rows]

    def step_of(step, carry):
        visit(step)
        return carry

    lax.fori_loop(0, slot_count - 1, step_of, 0)
    visit(slot_count - 1, final=True)
    settle(block - 1, theirs)
    hand_over(block - 1)
    settle(block - 1, mine)
    for slot in range(1, slot_count):
        for chunk in range(chunks):
            remote(piece, slot, beside, chunk).wait_send()
    for chunk in range(chunks):
        give(chunk).wait_send()
        join(other, 0, chunk).wait_send()
        join(core, 1, chunk).wait_send()
    sent = outbox.at[:, pl.ds(0, norb - block)]
    pltpu.make_async_copy(sent, sent, spread_sems.at[chunks]).wait()
    for i in range(block):
        swap(i).wait()
        out_ref[i] = acc[i, mine] + incoming[i].astype(f32)


def shards(ints, occ_coef, vir_coef, occ_energy, vir_energy):
    aux_count = lax.axis_size("aux")
    ao_count = lax.axis_size("ao")
    held, part, nao = ints.shape
    norb, nvir = occ_coef.shape[1], vir_coef.shape[1]
    block, half, naux = norb // aux_count, nvir // ao_count, held * aux_count
    share = block // ao_count
    slot_count = 2 * CYCLE + 1
    groups, chunks = 4, 2
    depth = held // chunks
    f32, bf16 = jnp.float32, jnp.bfloat16
    anywhere = pl.BlockSpec(memory_space=pl.ANY)
    dma = pltpu.SemaphoreType.DMA
    operands = (ints.reshape(held * part, nao), occ_coef.T, vir_coef, occ_energy, vir_energy[None, :])
    return pl.pallas_call(
        functools.partial(density_kernel, aux_count, share),
        out_shape=jax.ShapeDtypeStruct((block, half, nvir), f32),
        in_specs=[anywhere] * 5,
        out_specs=pl.BlockSpec(memory_space=pltpu.VMEM),
        scratch_shapes=[
            pltpu.VMEM((groups, held // groups * part, nao), bf16),
            pltpu.VMEM((norb, nao), bf16),
            pltpu.VMEM((part, nvir), bf16),
            pltpu.SMEM((norb,), f32),
            pltpu.VMEM((1, nvir), f32),
            pltpu.VMEM((chunks, depth * norb, part), bf16),
            pltpu.VMEM((chunks, depth * norb, half), bf16),
            pltpu.VMEM((chunks, depth * norb, half), bf16),
            pltpu.VMEM((chunks, depth * norb, half), f32),
            pltpu.VMEM((chunks, norb, depth, half), bf16),
            pltpu.VMEM((block, naux, nvir), bf16),
            pltpu.VMEM((slot_count, share, naux, nvir), bf16),
            pltpu.VMEM((block, nvir, naux), bf16),
            pltpu.VMEM((nvir, nvir), f32),
            pltpu.VMEM((block, nvir, nvir), bf16),
            pltpu.VMEM((block, nvir, nvir), bf16),
            pltpu.VMEM((block, nvir, nvir), f32),
            pltpu.VMEM((block, half, nvir), bf16),
            pltpu.VMEM((block, half, nvir), bf16),
            dma((groups,)),
            dma((4,)),
            dma((chunks,)),
            dma((chunks,)),
            dma((chunks + 1,)),
            dma((2, 2, chunks)),
            dma((slot_count, chunks)),
            dma((slot_count, chunks)),
            dma((2, block)),
        ],
        compiler_params=pltpu.CompilerParams(collective_id=0, has_side_effects=True, vmem_limit_bytes=44 * 2**20),
    )(*(pltpu.with_memory_space_constraint(operand, pltpu.HBM) for operand in operands))


def solution(mesh):
    return jax.shard_map(
        shards,
        mesh=mesh,
        in_specs=(P("aux", "ao", None), P(), P("ao", None), P(), P()),
        out_specs=P("aux", "ao", None),
        check_vma=False,
    )
```

```python
import functools

import jax
import jax.numpy as jnp
from jax import lax
from jax.experimental import pallas as pl
from jax.experimental.pallas import tpu as pltpu
from jax.sharding import PartitionSpec as P

CYCLE = 4
MESH = pl.DeviceIdType.MESH


def places(me, aux_count):
    layers = aux_count // CYCLE
    layer, place = lax.div(me, CYCLE), lax.rem(me, CYCLE)
    column, row = lax.rem(place, 2), lax.div(place, 2)
    base = layer * CYCLE
    beside = base + place + 1 - 2 * column
    along = base + place + 2 - 4 * row
    across = base + CYCLE - 1 - place
    above = lax.rem(me + CYCLE, aux_count)
    below = lax.rem(me + aux_count - CYCLE, aux_count)
    last = jnp.where(layer == layers - 1, 1, 0)
    bottom = jnp.where(layer == 0, 1, 0)
    return column, row, beside, along, across, above, below, bottom, last


def density_kernel(
    aux_count, share, ints_ref, occ_ref, vir_ref, occ_energy_ref, vir_energy_ref, out_ref,
    ints, occ_t, vir, occ_energy, vir_energy, half_ints, given, taken, kept, outbox, own,
    slots, own_t, vir_pairs, amp, mix, acc, outgoing, incoming,
    load_sems, input_sems, give_sems, take_sems, spread_sems, join_sems,
    send_sems, recv_sems, swap_sems,
):
    me = lax.axis_index("aux")
    core = lax.axis_index("ao")
    other = 1 - core
    block, naux, nvir = own.shape
    groups, rows_in_group, nao = ints.shape
    chunks, norb, depth, half = outbox.shape
    part = half_ints.shape[2]
    deep = naux // chunks
    slot_count = 2 * CYCLE + 1
    column, row, beside, along, across, above, below, bottom, last = places(me, aux_count)
    f32, bf16 = jnp.float32, jnp.bfloat16

    inputs = [
        pltpu.make_async_copy(source, target, input_sems.at[at])
        for at, (source, target) in enumerate(
            ((occ_ref, occ_t), (vir_ref, vir), (vir_energy_ref, vir_energy), (occ_energy_ref, occ_energy))
        )
    ]
    loads = [
        pltpu.make_async_copy(
            ints_ref.at[pl.ds(group * rows_in_group, rows_in_group)], ints.at[group], load_sems.at[group]
        )
        for group in range(groups)
    ]
    inputs[0].start()
    loads[0].start()
    for copy in inputs[1:] + loads[1:]:
        copy.start()

    barrier = pltpu.get_barrier_semaphore()

    def greet(step, carry):
        target = lax.rem(me + step, aux_count)
        pl.semaphore_signal(barrier, inc=1, device_id=(target, core), device_id_type=MESH)
        return carry

    lax.fori_loop(1, aux_count, greet, 0)
    pl.semaphore_signal(barrier, inc=1, device_id=(me, other), device_id_type=MESH)

    inputs[0].wait()
    occ = occ_t[...].T
    acc[...] = jnp.zeros_like(acc)
    amp[block - 1] = jnp.zeros_like(amp[block - 1])
    mix[block - 1] = jnp.zeros_like(mix[block - 1])
    inputs[1].wait()
    mine = pl.ds(pl.multiple_of(core * half, half), half)
    theirs = pl.ds(pl.multiple_of(other * half, half), half)
    to_row = lax.broadcasted_iota(jnp.int32, (norb * depth, norb * depth), 0)
    from_row = lax.broadcasted_iota(jnp.int32, (norb * depth, norb * depth), 1)
    order = jnp.where(from_row == lax.rem(to_row, depth) * norb + lax.div(to_row, depth), 1.0, 0.0).astype(bf16)

    def give(chunk):
        return pltpu.make_async_remote_copy(
            src_ref=given.at[chunk],
            dst_ref=taken.at[chunk],
            send_sem=give_sems.at[chunk],
            recv_sem=take_sems.at[chunk],
            device_id=(me, other),
            device_id_type=MESH,
        )

    def spread(chunk):
        give(chunk).wait_recv()
        total = kept[chunk] + taken[chunk].astype(f32)
        outbox[chunk] = total.astype(bf16).reshape(norb, depth, half)
        place = pl.ds(pl.multiple_of(chunk * deep + me * depth, depth), depth)

        def send(step, carry):
            target = lax.rem(me + step, aux_count)
            pltpu.make_async_remote_copy(
                src_ref=outbox.at[chunk, pl.ds(target * block, block)],
                dst_ref=own.at[:, place, mine],
                send_sem=spread_sems.at[chunks],
                recv_sem=spread_sems.at[chunk],
                device_id=(target, core),
                device_id_type=MESH,
            ).start()
            return carry

        lax.fori_loop(1, aux_count, send, 0)
        pltpu.make_async_copy(
            outbox.at[chunk, pl.ds(me * block, block)], own.at[:, place, mine], spread_sems.at[chunk]
        ).start()

    in_chunk = groups // chunks
    in_group = rows_in_group // part
    cut = rows_in_group // 2
    for group in range(groups):
        chunk = group // in_chunk
        loads[group].wait()
        for piece in range(2):
            product = jnp.dot(ints[group, piece * cut : (piece + 1) * cut], occ, preferred_element_type=f32).astype(bf16)
            for q in range(in_group // 2):
                at = ((group % in_chunk) * in_group + piece * (in_group // 2) + q) * norb
                half_ints[chunk, at : at + norb] = product[q * part : (q + 1) * part].T
        if group % in_chunk == in_chunk - 1:
            ordered = jnp.dot(order, half_ints[chunk], preferred_element_type=f32).astype(bf16)
            given[chunk] = jnp.dot(ordered, vir[:, theirs], preferred_element_type=f32).astype(bf16)
            if chunk == 0:
                pl.semaphore_wait(barrier, aux_count)
            give(chunk).start()
            kept[chunk] = jnp.dot(ordered, vir[:, mine], preferred_element_type=f32)
        elif chunk > 0 and group % in_chunk == 0:
            spread(chunk - 1)
    spread(chunks - 1)

    inputs[2].wait()
    inputs[3].wait()
    lanes = 128
    column_energy = jnp.broadcast_to(vir_energy[...], (lanes, nvir)).T
    vir_pairs[...] = jnp.concatenate([column_energy] * (nvir // lanes), axis=1) + vir_energy[...]

    def span(chunk):
        return pl.ds(chunk * deep, deep)

    def remote(source, slot, target, chunk, columns=slice(None)):
        return pltpu.make_async_remote_copy(
            src_ref=source.at[:, span(chunk), columns],
            dst_ref=slots.at[slot, :, span(chunk), columns],
            send_sem=send_sems.at[slot, chunk],
            recv_sem=recv_sems.at[slot, chunk],
            device_id=(target, core),
            device_id_type=MESH,
        )

    def arrived(slot, chunk):
        region = slots.at[slot, :, span(chunk)]
        pltpu.make_async_copy(region, region, recv_sems.at[slot, chunk]).wait()

    def join(orbital, at, chunk):
        half_block = own.at[pl.ds(orbital * share, share), span(chunk), mine]
        return pltpu.make_async_remote_copy(
            src_ref=half_block,
            dst_ref=half_block,
            send_sem=join_sems.at[0, at, chunk],
            recv_sem=join_sems.at[1, at, chunk],
            device_id=(me, other),
            device_id_type=MESH,
        )

    piece = own.at[pl.ds(core * share, share)]
    first = jnp.where(last == 1, above, below)
    second = jnp.where(last == 1, below, above)
    for chunk in range(chunks):
        own_half = own.at[:, span(chunk), mine]
        pltpu.make_async_copy(own_half, own_half, spread_sems.at[chunk]).wait()
        join(other, 0, chunk).start()
        for columns in (mine, theirs):
            remote(piece, 3, across, chunk, columns).start()
            remote(piece, 4 + last, first, chunk, columns).start()
            if columns is mine:
                join(core, 1, chunk).start()
                join(core, 0, chunk).wait_recv()
        remote(piece, 5 - last, second, chunk).start()
        if chunk == 0:
            remote(piece, 1, beside, chunk).start()
            remote(piece, 2, along, chunk).start()
        pltpu.make_async_copy(
            piece.at[:, span(chunk)], slots.at[0, :, span(chunk)], recv_sems.at[0, chunk]
        ).start()
    beside_source, along_source = 4 + column, 4 + row
    beyond = jnp.where(row == 0, above, below)
    for chunk in range(chunks):
        join(other, 1, chunk).wait_recv()

    for i in range(block):
        own_t[i] = own[i].T

    early, late = 4 + bottom, 5 - bottom

    def forward(source, chunk):
        @pl.when(beside_source == source)
        def _():
            remote(slots.at[source], 6, beside, chunk).start()

        @pl.when(along_source == source)
        def _():
            remote(slots.at[source], 7, along, chunk).start()

    def settle(i, rows=slice(None)):
        acc[i, rows] += jnp.dot(amp[i, rows], mix[i], preferred_element_type=f32)

    def swap(i):
        return pltpu.make_async_remote_copy(
            src_ref=outgoing.at[i],
            dst_ref=incoming.at[i],
            send_sem=swap_sems.at[0, i],
            recv_sem=swap_sems.at[1, i],
            device_id=(me, other),
            device_id_type=MESH,
        )

    def hand_over(i):
        outgoing[i] = acc[i, theirs].astype(bf16)
        swap(i).start()

    tiles = [slice(0, half), slice(half, nvir)]

    def visit(step, final=False):
        slot = jnp.where(step == 1, 3, jnp.where(step == 2, early, jnp.where(step == 3, late, step)))
        slot = jnp.where(step == 4, 1, jnp.where(step == 5, 2, slot))

        @pl.when(step == 1)
        def _():
            arrived(3, 0)
            remote(slots.at[3], 8, beyond, 0).start()
            remote(piece, 1, beside, 1).start()
            remote(piece, 2, along, 1).start()
            for source in (early, late):
                arrived(source, 0)
                forward(source, 0)
            arrived(3, 1)
            remote(slots.at[3], 8, beyond, 1).start()

        @pl.when(step == 2)
        def _():
            arrived(early, 1)
            forward(early, 1)

        @pl.when(step == 3)
        def _():
            arrived(late, 1)
            forward(late, 1)

        @pl.when((step < 1) | (step > 3))
        def _():
            for chunk in range(chunks):
                arrived(slot, chunk)

        to_owner = jnp.where(slot == 0, me, jnp.where(slot == 1, beside, jnp.where(slot == 2, along, across)))
        from_beside = jnp.where(column == 1, beside + CYCLE, beside + aux_count - CYCLE)
        from_along = jnp.where(row == 1, along + CYCLE, along + aux_count - CYCLE)
        from_beyond = jnp.where(row == 1, across + CYCLE, across + aux_count - CYCLE)
        forwarded = jnp.where(slot == 6, from_beside, jnp.where(slot == 7, from_along, from_beyond))
        forwarded = lax.rem(forwarded, aux_count)
        stacked = jnp.where(slot == 4, above, below)
        owner = jnp.where(slot < 4, to_owner, jnp.where(slot < 6, stacked, forwarded))
        for s in range(share):
            pair_energy = occ_energy[owner * block + core * share + s]
            visitor = slots[slot, s]
            for i in range(block):
                energy = occ_energy[me * block + i] + pair_energy
                for rows in tiles:
                    direct = jnp.dot(own_t[i, rows], visitor, preferred_element_type=f32)
                    amp[i, rows] = (direct * (1.0 / (energy - vir_pairs[rows]))).astype(bf16)
                settle((i - 1) % block)
                if final and s == share - 1 and i > 0:
                    hand_over(i - 1)
                for rows in tiles:
                    mix[i, rows] = 2 * amp[i, :, rows].T - amp[i, rows]

    def step_of(step, carry):
        visit(step)
        return carry

    lax.fori_loop(0, slot_count - 1, step_of, 0)
    visit(slot_count - 1, final=True)
    settle(block - 1, theirs)
    hand_over(block - 1)
    settle(block - 1, mine)
    for slot in range(1, slot_count):
        for chunk in range(chunks):
            remote(piece, slot, beside, chunk).wait_send()
    for chunk in range(chunks):
        give(chunk).wait_send()
        join(other, 0, chunk).wait_send()
        join(core, 1, chunk).wait_send()
    sent = outbox.at[:, pl.ds(0, norb - block)]
    pltpu.make_async_copy(sent, sent, spread_sems.at[chunks]).wait()
    for i in range(block):
        swap(i).wait()
        out_ref[i] = acc[i, mine] + incoming[i].astype(f32)


def shards(ints, occ_coef, vir_coef, occ_energy, vir_energy):
    aux_count = lax.axis_size("aux")
    ao_count = lax.axis_size("ao")
    held, part, nao = ints.shape
    norb, nvir = occ_coef.shape[1], vir_coef.shape[1]
    block, half, naux = norb // aux_count, nvir // ao_count, held * aux_count
    share = block // ao_count
    slot_count = 2 * CYCLE + 1
    groups, chunks = 4, 2
    depth = held // chunks
    f32, bf16 = jnp.float32, jnp.bfloat16
    anywhere = pl.BlockSpec(memory_space=pl.ANY)
    dma = pltpu.SemaphoreType.DMA
    operands = (ints.reshape(held * part, nao), occ_coef.T, vir_coef, occ_energy, vir_energy[None, :])
    return pl.pallas_call(
        functools.partial(density_kernel, aux_count, share),
        out_shape=jax.ShapeDtypeStruct((block, half, nvir), f32),
        in_specs=[anywhere] * 5,
        out_specs=pl.BlockSpec(memory_space=pltpu.VMEM),
        scratch_shapes=[
            pltpu.VMEM((groups, held // groups * part, nao), bf16),
            pltpu.VMEM((norb, nao), bf16),
            pltpu.VMEM((part, nvir), bf16),
            pltpu.SMEM((norb,), f32),
            pltpu.VMEM((1, nvir), f32),
            pltpu.VMEM((chunks, depth * norb, part), bf16),
            pltpu.VMEM((chunks, depth * norb, half), bf16),
            pltpu.VMEM((chunks, depth * norb, half), bf16),
            pltpu.VMEM((chunks, depth * norb, half), f32),
            pltpu.VMEM((chunks, norb, depth, half), bf16),
            pltpu.VMEM((block, naux, nvir), bf16),
            pltpu.VMEM((slot_count, share, naux, nvir), bf16),
            pltpu.VMEM((block, nvir, naux), bf16),
            pltpu.VMEM((nvir, nvir), f32),
            pltpu.VMEM((block, nvir, nvir), bf16),
            pltpu.VMEM((block, nvir, nvir), bf16),
            pltpu.VMEM((block, nvir, nvir), f32),
            pltpu.VMEM((block, half, nvir), bf16),
            pltpu.VMEM((block, half, nvir), bf16),
            dma((groups,)),
            dma((4,)),
            dma((chunks,)),
            dma((chunks,)),
            dma((chunks + 1,)),
            dma((2, 2, chunks)),
            dma((slot_count, chunks)),
            dma((slot_count, chunks)),
            dma((2, block)),
        ],
        compiler_params=pltpu.CompilerParams(collective_id=0, has_side_effects=True, vmem_limit_bytes=44 * 2**20),
    )(*(pltpu.with_memory_space_constraint(operand, pltpu.HBM) for operand in operands))


def solution(mesh):
    return jax.shard_map(
        shards,
        mesh=mesh,
        in_specs=(P("aux", "ao", None), P(), P("ao", None), P(), P()),
        out_specs=P("aux", "ao", None),
        check_vma=False,
    )
```
